512 devices in a mesh: groups: 2 (over y), seq: 32 (over z), tp: 4 (over x), sub: 2 (over core).
Axes of the slice: x: 4, y: 2, z: 32, core: 2. Of those that a mesh axis runs over, the one named last changes fastest.
The devices are a block of a 4x8x32 slice.
Arguments:
- prefill_kv: bfloat16 [1024, 2, 128, 1024], P(('groups', 'seq'), None, ('tp', 'sub')), parts along dimension 0, may hold values from -7 to 7
- prompt_lengths: int32 [128], P('groups'), parts along dimension 0, may hold values from 1 to 3584, 57344 in all
- block_owner: int32 [1024], P('groups'), parts along dimension 0, may hold values from 0 to 31, as said below
- slot_order: int32 [64, 40], P('groups'), parts along dimension 0, may hold values from 0 to 39, each once within a row
- queries: bfloat16 [128, 8192], P('groups', ('tp', 'sub')), parts along dimension 0, may hold values from -10 to 10
- new_kv: bfloat16 [128, 2, 1024], P('groups', None, ('tp', 'sub')), parts along dimension 0, may hold values from -6 to 6
Outputs:
- decode_cache: bfloat16 [2560, 2, 128, 1024], P(('groups', 'seq'), None, None, ('tp', 'sub')), parts along dimension 0
- attention: bfloat16 [128, 8192], P('groups', ('tp', 'sub')), parts along dimension 0
The draws below stay inside these ranges and needn't reach their ends.
There are 2 independent parts, one for each index of `groups`. The reference program is written for one: setup_inputs(seed, part) draws one part's arguments, and reference() takes and returns one part's arrays. A program takes and returns all parts, laid end to end along the dimension named above; each array names one. Nothing has to cross between parts.
Inputs may be any that keep to these rules, and one draw needn't show every extreme that they name: `prompt_lengths`: they sum to 57344, and one equals 3584. `block_owner`: of the 16 blocks of one prefill shard (blocks s * 16 to s * 16 + 15), at most 2 name the same owner, and some shard reaches it; every owner is named by at most 40 blocks, and some owner by exactly 40.
All inputs are finite; a program needn't handle non-finite values.
Results may differ from the reference program's by a relative error of at most 0.003.
Values may be sent and summed in bfloat16 or wider, within the bound.
A program may use at most 64 MiB of HBM per device.

```python
import math
import jax
import jax.numpy as jnp
import numpy as np
from jax import lax

QH = 64
KVH = 8
HD = 128
BLOCK = 128
BLK_DEV = 16
NBLK = 512
REQUESTS = 64
CAP = 40
LONGEST = 3584
N_SEQ = 32


def draw_prefill_kv(key, part):
    base = jax.random.truncated_normal(jax.random.fold_in(key, 12), -4.0, 4.0, (NBLK, 2, BLOCK, KVH, HD), jnp.float32)
    return base.reshape(NBLK, 2, BLOCK, KVH * HD).astype(jnp.bfloat16)


def draw_queries(key, part):
    noise = jax.random.truncated_normal(jax.random.fold_in(key, 14), -4.0, 4.0, (REQUESTS, QH, HD), jnp.float32)
    values = 2.5 * noise
    return values.reshape(REQUESTS, QH * HD).astype(jnp.bfloat16)


def draw_block_owner(key, part):
    quarter = N_SEQ // 4
    half = BLK_DEV // 2
    pick = jax.random.randint(jax.random.fold_in(key, 21), (), 0, quarter)
    shard = jnp.arange(N_SEQ, dtype=jnp.int32)[:, None]
    column = jnp.arange(BLK_DEV, dtype=jnp.int32)[None, :]
    first = (shard + 4 * pick + column) % N_SEQ
    second = 4 * ((shard + pick + column - half) % quarter)
    target = jnp.where(column < half, first, second)
    shard_keys = jax.random.split(jax.random.fold_in(key, 22), N_SEQ)
    order = jax.vmap(lambda k: jax.random.permutation(k, BLK_DEV))(shard_keys)
    target = jnp.take_along_axis(target, order, axis=1)
    relabel = jax.random.permutation(jax.random.fold_in(key, 23), N_SEQ)
    return relabel[target].reshape(-1).astype(jnp.int32)


def block_scale(key, shape, cuts, smallest, high):
    level, own = 1.0, jax.random.fold_in(key, 6)
    for position, parts in cuts:
        draws = jnp.exp(jax.random.uniform(jax.random.fold_in(own, position), (parts,), jnp.float32, smallest / len(cuts), high / len(cuts)))
        level = level * jnp.repeat(draws, shape[position] // parts).reshape([-1 if axis == position else 1 for axis in range(len(shape))])
    return level


def split_up(count, total, limit, slope):
    weights = [(1 << 20) // math.isqrt(standing ** slope) + 1 for standing in range(2, count + 1)]
    rest, given = total - limit - (count - 1), [1] * (count - 1)
    while rest > 0:
        candidates = [i for i in range(count - 1) if given[i] < limit]
        mass, left = sum([weights[i] for i in candidates]), rest
        for i in candidates:
            more = min(limit - given[i], max(1, left * weights[i] // mass), rest)
            given[i] = given[i] + more
            rest = rest - more
    return np.array([limit] + given)


def ragged_sizes(key, count, total, limit, skew):
    if count == 2:
        one = jax.random.randint(key, (), max(1, total - limit), min(limit, total - 1) + 1)
        return jnp.stack([one, total - one])
    lengths = jnp.asarray(split_up(count, total, limit, skew), jnp.int32)
    pairs = (count - 1) // 2
    source_of, sink = lengths[1:1 + 2 * pairs:2], lengths[2:2 + 2 * pairs:2]
    room = jnp.minimum(source_of - 1, limit - sink)
    moved = jax.random.randint(jax.random.fold_in(key, 1), (pairs,), 0, 1 << 20) % (room + 1)
    lengths = lengths.at[1:1 + 2 * pairs:2].set(source_of - moved).at[2:2 + 2 * pairs:2].set(sink + moved)
    return lengths[jax.random.permutation(jax.random.fold_in(key, 2), count)]


def gaussian(stream_key, extent, scale, limit, shards=(), held_as=jnp.bfloat16):
    values = jax.random.normal(stream_key, extent, jnp.float32) * scale
    if len(shards) > 0:
        values = block_scale(stream_key, extent, shards, -0.22, 0.18) * values
    return jnp.clip(values, min=-limit, max=limit).astype(held_as)


def setup_inputs(seed: int = 0, part: int = 0) -> dict:
    keys = jax.random.split(jax.random.key(seed), 7)
    own_keys = jax.random.split(jax.random.fold_in(keys[6], part), 7)
    prefill_kv = draw_prefill_kv(jax.random.fold_in(jax.random.fold_in(keys[6], part), 71), part)
    prompt_lengths = ragged_sizes(own_keys[1], REQUESTS, BLOCK * (NBLK - REQUESTS), LONGEST, 2).astype(jnp.int32)
    block_owner = draw_block_owner(jax.random.fold_in(jax.random.fold_in(keys[6], part), 71), part)
    slot_order = jax.vmap(lambda own: jax.random.permutation(own, CAP))(jax.random.split(own_keys[3], N_SEQ)).reshape((N_SEQ, CAP)).astype(jnp.int32)
    queries = draw_queries(jax.random.fold_in(jax.random.fold_in(keys[6], part), 71), part)
    new_kv = gaussian(own_keys[5], (REQUESTS, 2, KVH * HD), 1.0, 6.0, ((2, 8),))
    return {"prefill_kv": prefill_kv, "prompt_lengths": prompt_lengths, "block_owner": block_owner, "slot_order": slot_order, "queries": queries, "new_kv": new_kv}


NEG_FLOOR = -1e30


def layout(prompt_lengths, global_ids, live_rows):
    counts = (prompt_lengths + BLOCK - 1) // BLOCK
    block_ends = jnp.cumsum(counts).astype(jnp.int32)
    starts = block_ends - counts
    member = (global_ids[None, :] >= starts[:, None]) & (global_ids[None, :] < block_ends[:, None]) & live_rows[None, :]
    remaining = prompt_lengths[:, None] - (global_ids[None, :] - starts[:, None]) * BLOCK
    valid_rows = jnp.sum(jnp.where(member, jnp.clip(remaining, 0, BLOCK), 0), axis=0).astype(jnp.int32)
    return member, valid_rows


def block_terms(blocks, member, valid_rows, queries):
    block_count = blocks.shape[0]
    head_count = blocks.shape[3] // HD
    group_size = queries.shape[1] // (head_count * HD)
    selector = member.T.astype(jnp.bfloat16)
    picked = jnp.dot(selector, queries, preferred_element_type=jnp.float32).astype(jnp.bfloat16)
    picked = picked.reshape(block_count, head_count, group_size, HD).astype(jnp.float32)
    key_rows = blocks[:, 0].reshape(block_count, BLOCK, head_count, HD).astype(jnp.float32)
    value_rows = blocks[:, 1].reshape(block_count, BLOCK, head_count, HD).astype(jnp.float32)
    scores = jnp.einsum('xhgd,xthd->xhgt', picked, key_rows, precision=lax.Precision.HIGHEST) * (HD ** -0.5)
    live_tokens = jnp.arange(BLOCK)[None, :] < valid_rows[:, None]
    scores = jnp.where(live_tokens[:, None, None, :], scores, NEG_FLOOR)
    block_peak = jnp.max(scores, axis=-1)
    weight = jnp.exp(scores - block_peak[..., None]).astype(jnp.bfloat16)
    weight_sum = jnp.sum(weight.astype(jnp.float32), axis=-1)
    weighted = jnp.einsum('xhgt,xthd->xhgd', weight.astype(jnp.float32), value_rows, precision=lax.Precision.HIGHEST)
    inside = member[:, :, None, None]
    highest = jnp.max(jnp.where(inside, block_peak[None], NEG_FLOOR), axis=1)
    rescale = jnp.where(inside, jnp.exp(block_peak[None] - highest[:, None]), 0.0)
    totals = jnp.sum(rescale * weight_sum[None], axis=1)
    outputs = jnp.einsum('rxhg,xhgd->rhgd', rescale, weighted, precision=lax.Precision.HIGHEST)
    return highest, totals, outputs


def finish(highest, totals, outputs, queries, new_kv):
    request_count = queries.shape[0]
    head_count = new_kv.shape[2] // HD
    group_size = queries.shape[1] // (head_count * HD)
    query_rows = queries.reshape(request_count, head_count, group_size, HD).astype(jnp.float32)
    new_keys = new_kv[:, 0].reshape(request_count, head_count, HD).astype(jnp.float32)
    new_values = new_kv[:, 1].reshape(request_count, head_count, HD).astype(jnp.float32)
    own_score = jnp.einsum('rhgd,rhd->rhg', query_rows, new_keys, precision=lax.Precision.HIGHEST) * (HD ** -0.5)
    summit = jnp.maximum(highest, own_score)
    cache_part = jnp.exp(highest - summit)
    own_part = jnp.exp(own_score - summit)
    numer = cache_part[..., None] * outputs + own_part[..., None] * new_values[:, :, None, :]
    denom = cache_part * totals + own_part
    return (numer / denom[..., None]).reshape(request_count, -1).astype(jnp.bfloat16)


def reference(prefill_kv, prompt_lengths, block_owner, slot_order, queries, new_kv):
    block_total = block_owner.shape[0]
    capacity = slot_order.shape[1]
    owner_ids = jnp.arange(N_SEQ, dtype=jnp.int32)
    owner_hot = (block_owner[:, None] == owner_ids[None, :]).astype(jnp.int32)
    owner_rank = jnp.sum((jnp.cumsum(owner_hot, axis=0) - owner_hot) * owner_hot, axis=1).astype(jnp.int32)
    cache_slot = slot_order[block_owner, owner_rank].astype(jnp.int32)
    target_rows = (block_owner * capacity + cache_slot).astype(jnp.int32)
    decode_cache = jnp.zeros((N_SEQ * capacity,) + prefill_kv.shape[1:], jnp.bfloat16).at[target_rows].set(prefill_kv)
    global_ids = jnp.arange(block_total, dtype=jnp.int32)
    member, valid_rows = layout(prompt_lengths, global_ids, jnp.ones((block_total,), bool))
    highest, totals, outputs = block_terms(prefill_kv, member, valid_rows, queries)
    attention = finish(highest, totals, outputs, queries, new_kv)
    return decode_cache, attention
```

```python
import functools

import jax
import jax.numpy as jnp
from jax import lax
from jax.experimental import pallas as pl
from jax.experimental.pallas import tpu as pltpu
from jax.sharding import PartitionSpec as P

HD = 128
BLOCK = 128
NEG_FLOOR = -1e30
MESH = pl.DeviceIdType.MESH
SPLITS = (13, 14, 15, 16, 17, 18)


def loads(steps_of_slot):
    return tuple(sum(c >= k for c in steps_of_slot) for k in range(1, max(steps_of_slot) + 1))


def tiers(shard_blocks, seq):
    half = seq // 2
    picks = [
        [18, 17, 15, 14, 12, 11, 9, 8, 6, 5, 3],
        [18, 17, 15, 14, 13, 12, 10, 9, 8, 6, 5, 4, 2],
    ]
    every = [half - i // 2 for i in range(shard_blocks)]
    return tuple(loads(p) for p in picks) + (loads(every),)


def exchange_kernel(tp, sub, groups, x_ref, tier_ref, own_ref, tiers_ref, sem, send_sem, recv_sem, tier_send, tier_recv):
    width = own_ref.shape[3]
    rows = x_ref.shape[2]
    count = tp * sub
    me = lax.axis_index("tp") * sub + lax.axis_index("sub")
    group = lax.axis_index("groups")

    def peer(step):
        other = lax.rem(me + step, count)
        return other, {"tp": other // sub, "sub": lax.rem(other, sub)}

    barrier = pltpu.get_barrier_semaphore()
    for step in range(1, count):
        pl.semaphore_signal(barrier, inc=1, device_id=peer(step)[1], device_id_type=MESH)
    for step in range(1, groups):
        pl.semaphore_signal(barrier, inc=1, device_id={"groups": lax.rem(group + step, groups)}, device_id_type=MESH)
    pl.semaphore_wait(barrier, count + groups - 2)

    mine = pl.ds(pl.multiple_of(me * rows, rows), rows)
    copies = []
    for step in range(1, groups):
        copies.append(
            pltpu.make_async_remote_copy(
                src_ref=tier_ref,
                dst_ref=tiers_ref.at[group],
                send_sem=tier_send.at[step],
                recv_sem=tier_recv.at[step],
                device_id={"groups": lax.rem(group + step, groups)},
                device_id_type=MESH,
            )
        )
    for step in range(1, count):
        other, where = peer(step)
        copies.append(
            pltpu.make_async_remote_copy(
                src_ref=x_ref.at[:, :, :, pl.ds(pl.multiple_of(other * width, width), width)],
                dst_ref=own_ref.at[:, :, mine, :],
                send_sem=send_sem.at[step],
                recv_sem=recv_sem.at[step],
                device_id=where,
                device_id_type=MESH,
            )
        )
    for copy in copies:
        copy.start()
    local = pltpu.make_async_copy(
        x_ref.at[:, :, :, pl.ds(pl.multiple_of(me * width, width), width)], own_ref.at[:, :, mine, :], sem
    )
    local.start()
    tiers_ref[group] = tier_ref[...]
    local.wait()
    for copy in copies:
        copy.wait()


def exchange(prefill_kv, tier, tp, sub, groups):
    blocks, two, rows, columns = prefill_kv.shape
    count = tp * sub
    return pl.pallas_call(
        functools.partial(exchange_kernel, tp, sub, groups),
        out_shape=(
            jax.ShapeDtypeStruct((blocks, two, rows * count, columns // count), prefill_kv.dtype),
            jax.ShapeDtypeStruct((groups, 8, 128), jnp.int32),
        ),
        in_specs=[pl.BlockSpec(memory_space=pl.ANY), pl.BlockSpec(memory_space=pltpu.VMEM)],
        out_specs=[pl.BlockSpec(memory_space=pltpu.VMEM)] * 2,
        scratch_shapes=[
            pltpu.SemaphoreType.DMA,
            pltpu.SemaphoreType.DMA((count,)),
            pltpu.SemaphoreType.DMA((count,)),
            pltpu.SemaphoreType.DMA((groups,)),
            pltpu.SemaphoreType.DMA((groups,)),
        ],
        compiler_params=pltpu.CompilerParams(collective_id=0, has_side_effects=True),
    )(prefill_kv, jnp.broadcast_to(tier, (8, 128)))


def ring_kernel(
    used, seq, own_ref, att_ref, pick_ref, from_ref, row_ref, cache_ref, rows_ref,
    log, alog, send_sem, recv_sem, asend_sem, arecv_sem,
):
    me = lax.axis_index("seq")
    right, left = {"seq": lax.rem(me + 1, seq)}, {"seq": lax.rem(me + seq - 1, seq)}
    blocks = own_ref.shape[0]
    wide, total = used[0], sum(used)
    starts = [sum(used[:k]) for k in range(len(used))]
    stage = blocks + 1
    base = (stage + 2 * wide, stage + 2 * wide + total)
    slots = att_ref.shape[0]
    reach = (seq // 2, seq - 1 - seq // 2)

    log[blocks] = jnp.zeros(log.shape[1:], log.dtype)

    def keep(i, carry):
        log[i] = own_ref[i]
        return carry

    lax.fori_loop(0, blocks, keep, 0)

    def pick(i, carry):
        log[stage + i] = own_ref[pick_ref[i]]
        return carry

    lax.fori_loop(0, 2 * wide, pick, 0)
    alog[pl.ds(0, slots)] = att_ref[...]

    barrier = pltpu.get_barrier_semaphore()
    for where in (left, right):
        pl.semaphore_signal(barrier, inc=1, device_id=where, device_id_type=MESH)
    pl.semaphore_wait(barrier, 2)

    def block_copy(way, step, i):
        at = starts[step] + i
        source = stage + way * wide + i if step == 0 else base[way] + starts[step - 1] + i
        return pltpu.make_async_remote_copy(
            src_ref=log.at[source],
            dst_ref=log.at[base[way] + at],
            send_sem=send_sem.at[way, at],
            recv_sem=recv_sem.at[way, at],
            device_id=(right, left)[way],
            device_id_type=MESH,
        )

    def row_copy(way, step):
        at = way * reach[0] + step + 1
        source = att_ref if step == 0 else alog.at[pl.ds((at - 1) * slots, slots)]
        return pltpu.make_async_remote_copy(
            src_ref=source,
            dst_ref=alog.at[pl.ds(at * slots, slots)],
            send_sem=asend_sem.at[at],
            recv_sem=arecv_sem.at[at],
            device_id=(right, left)[way],
            device_id_type=MESH,
        )

    for step in range(max(len(used), reach[0])):
        for way in range(2):
            if step < reach[way]:
                if step > 0:
                    row_copy(way, step - 1).wait_recv()
                row_copy(way, step).start()
        if step < len(used):

            def forward(i, carry, step=step):
                for way in range(2):
                    if step > 0:
                        block_copy(way, step - 1, i).wait_recv()
                    block_copy(way, step, i).start()
                return carry

            lax.fori_loop(0, used[step], forward, 0)

    for step in range(len(used)):
        beyond = used[step + 1] if step + 1 < len(used) else 0

        def land(i, carry, step=step):
            for way in range(2):
                block_copy(way, step, i).wait_recv()
            return carry

        lax.fori_loop(beyond, used[step], land, 0)

        def sent(i, carry, step=step):
            for way in range(2):
                block_copy(way, step, i).wait_send()
            return carry

        lax.fori_loop(0, used[step], sent, 0)
    for way in range(2):
        row_copy(way, reach[way] - 1).wait_recv()
        for step in range(reach[way]):
            row_copy(way, step).wait_send()

    def place(c, carry):
        cache_ref[c] = log[from_ref[c]]
        return carry

    lax.fori_loop(0, cache_ref.shape[0], place, 0)

    def answer(r, carry):
        rows_ref[r] = alog[row_ref[r]]
        return carry

    lax.fori_loop(0, rows_ref.shape[0], answer, 0)


def ring(used, number, seq, capacity, requests, own, att, pick, source, row_source):
    blocks = own.shape[0]
    wide, total = used[0], sum(used)
    vmem = pl.BlockSpec(memory_space=pltpu.VMEM)
    smem = pl.BlockSpec(memory_space=pltpu.SMEM)
    return pl.pallas_call(
        functools.partial(ring_kernel, used, seq),
        out_shape=(
            jax.ShapeDtypeStruct((capacity,) + own.shape[1:], own.dtype),
            jax.ShapeDtypeStruct((requests,) + att.shape[1:], att.dtype),
        ),
        in_specs=[vmem, vmem, smem, smem, smem],
        out_specs=(vmem, vmem),
        scratch_shapes=[
            pltpu.VMEM((blocks + 1 + 2 * wide + 2 * total,) + own.shape[1:], own.dtype),
            pltpu.VMEM((seq * att.shape[0],) + att.shape[1:], att.dtype),
            pltpu.SemaphoreType.DMA((2, total)),
            pltpu.SemaphoreType.DMA((2, total)),
            pltpu.SemaphoreType.DMA((seq,)),
            pltpu.SemaphoreType.DMA((seq,)),
        ],
        compiler_params=pltpu.CompilerParams(
            collective_id=number, has_side_effects=True, vmem_limit_bytes=60 << 20
        ),
    )(own, att, pick, source, row_source)


def travel(used, slot):
    return sum((slot < n).astype(jnp.int32) for n in used)


def layout(prompt_lengths, global_ids, starts, block_ends):
    member = (global_ids[None, :] >= starts[:, None]) & (global_ids[None, :] < block_ends[:, None])
    remaining = prompt_lengths[:, None] - (global_ids[None, :] - starts[:, None]) * BLOCK
    valid_rows = jnp.sum(jnp.where(member, jnp.clip(remaining, 0, BLOCK), 0), axis=0)
    return (member, valid_rows)


def block_terms(blocks, member, valid_rows, queries):
    block_count = blocks.shape[0]
    head_count = blocks.shape[3] // HD
    group_size = queries.shape[1] // (head_count * HD)
    selector = member.T.astype(jnp.bfloat16)
    picked = jnp.dot(selector, queries, preferred_element_type=jnp.float32).astype(jnp.bfloat16)
    picked = picked.reshape(block_count, head_count, group_size, HD)
    key_rows = blocks[:, 0].reshape(block_count, BLOCK, head_count, HD)
    value_rows = blocks[:, 1].reshape(block_count, BLOCK, head_count, HD)
    scores = jnp.einsum(
        "xhgd,xthd->xhgt", picked, key_rows, preferred_element_type=jnp.float32
    ) * HD ** (-0.5)
    live_tokens = jnp.arange(BLOCK)[None, :] < valid_rows[:, None]
    scores = jnp.where(live_tokens[:, None, None, :], scores, NEG_FLOOR)
    block_peak = jnp.max(scores, axis=-1)
    weight = jnp.exp(scores - block_peak[..., None]).astype(jnp.bfloat16)
    weight_sum = jnp.sum(weight.astype(jnp.float32), axis=-1)
    weighted = jnp.einsum("xhgt,xthd->xhgd", weight, value_rows, preferred_element_type=jnp.float32)
    inside = member[:, :, None, None]
    highest = jnp.max(jnp.where(inside, block_peak[None], NEG_FLOOR), axis=1)
    rescale = jnp.where(inside, jnp.exp(block_peak[None] - highest[:, None]), 0.0)
    totals = jnp.sum(rescale * weight_sum[None], axis=1)
    outputs = jnp.einsum("rxhg,xhgd->rhgd", rescale, weighted, precision=lax.Precision.HIGHEST)
    return (highest, totals, outputs)


def finish(states, queries, new_kv):
    request_count = queries.shape[0]
    head_count = new_kv.shape[2] // HD
    group_size = queries.shape[1] // (head_count * HD)
    query_rows = queries.reshape(request_count, head_count, group_size, HD)
    new_keys = new_kv[:, 0].reshape(request_count, head_count, HD)
    new_values = new_kv[:, 1].reshape(request_count, head_count, HD).astype(jnp.float32)
    own_score = jnp.einsum(
        "rhgd,rhd->rhg", query_rows, new_keys, preferred_element_type=jnp.float32
    ) * HD ** (-0.5)
    summit = own_score
    for highest, _, _ in states:
        summit = jnp.maximum(summit, highest)
    own_part = jnp.exp(own_score - summit)
    numer = own_part[..., None] * new_values[:, :, None, :]
    denom = own_part
    for highest, totals, outputs in states:
        part = jnp.exp(highest - summit)
        numer = numer + part[..., None] * outputs
        denom = denom + part * totals
    return (numer / denom[..., None]).reshape(request_count, -1).astype(jnp.bfloat16)


def per_device(tp, sub, groups, seq, prefill_kv, prompt_lengths, block_owner, slot_order, queries, new_kv):
    me = lax.axis_index("seq")
    shard_blocks = prefill_kv.shape[0]
    capacity = slot_order.shape[1]
    requests = prompt_lengths.shape[0]
    schedules = tiers(shard_blocks, seq)

    owners = block_owner.reshape(seq, shard_blocks)
    shards = jnp.arange(seq, dtype=jnp.int32)
    ahead = lax.rem(owners - shards[:, None] + seq, seq)
    key = ahead * shard_blocks + jnp.arange(shard_blocks, dtype=jnp.int32)[None, :]
    order = jnp.sum((key[:, None, :] < key[:, :, None]).astype(jnp.int32), axis=2)
    split = jnp.array(SPLITS, jnp.int32)
    to_right = ahead[None] <= split[:, None, None]
    rightward = jnp.sum(to_right.astype(jnp.int32), axis=2, keepdims=True)
    slot = jnp.where(to_right, rightward - 1 - order[None], order[None] - rightward)
    steps = jnp.where(to_right, ahead[None], seq - ahead[None])
    steps = jnp.where(ahead[None] == 0, 0, steps)
    fits = jnp.stack([jnp.all(steps <= travel(used, slot), axis=2) for used in schedules])
    shard_fits = jnp.any(fits, axis=1)
    tier_fits = jnp.all(shard_fits, axis=1)
    own_tier = jnp.minimum(jnp.sum((~tier_fits).astype(jnp.int32)), len(schedules) - 1)

    own, agreed = exchange(prefill_kv, own_tier, tp, sub, groups)
    tier = jnp.max(agreed)

    counts = (prompt_lengths + BLOCK - 1) // BLOCK
    block_ends = jnp.cumsum(counts)
    block_starts = block_ends - counts
    low = me * shard_blocks
    member, valid_rows = layout(
        prompt_lengths, low + jnp.arange(shard_blocks, dtype=jnp.int32), block_starts, block_ends
    )
    highest, totals, outputs = block_terms(own, member, valid_rows, queries)

    def open_at(edge):
        return ((block_starts < edge) & (block_ends > edge) & (edge > 0))[:, None, None]

    leaving = open_at(low + shard_blocks)
    state = jnp.concatenate(
        [
            jnp.sum(jnp.where(leaving[..., None], outputs, 0.0), axis=0),
            jnp.broadcast_to(
                jnp.sum(jnp.where(leaving, highest, 0.0), axis=0)[..., None], outputs.shape[1:]
            ),
            jnp.broadcast_to(
                jnp.sum(jnp.where(leaving, totals, 0.0), axis=0)[..., None], outputs.shape[1:]
            ),
        ],
        axis=2,
    )
    states = [(highest, totals, outputs)]
    for back in (1, 2):
        came = lax.ppermute(state, "seq", [(s, (s + back) % seq) for s in range(seq)])
        entering = open_at(low - (back - 1) * shard_blocks)
        states.append(
            (
                jnp.where(entering, came[None, ..., HD], NEG_FLOOR),
                jnp.where(entering, came[None, ..., 2 * HD], 0.0),
                jnp.where(entering[..., None], came[None, ..., :HD], 0.0),
            )
        )
    attention = finish(states, queries, new_kv)
    last_shard = (block_ends - 1) // shard_blocks
    first_done = jnp.sum((last_shard < me).astype(jnp.int32))
    done = lax.dynamic_slice_in_dim(
        jnp.pad(attention, ((0, shard_blocks), (0, 0))), first_done, shard_blocks
    ).reshape(shard_blocks, -1, HD)
    ids = jnp.arange(requests, dtype=jnp.int32)
    place = jnp.sum(
        ((last_shard[:, None] == last_shard[None, :]) & (ids[None, :] < ids[:, None])).astype(jnp.int32), axis=1
    )
    behind = lax.rem(me - last_shard + seq, seq)
    half = seq // 2
    row_source = jnp.where(behind <= half, behind, half + seq - behind) * shard_blocks + place

    mine = block_owner == me
    rank = jnp.cumsum(mine.astype(jnp.int32)) - 1
    own_slots = lax.dynamic_slice_in_dim(slot_order, me, 1)[0]
    nth = mine[None, :] & (rank[None, :] == jnp.arange(capacity, dtype=jnp.int32)[:, None])
    row_of = own_slots[:, None] == jnp.arange(capacity, dtype=jnp.int32)[None, :]

    def deliver(number):
        used = schedules[number]
        choice = fits[number]
        first = jnp.argmax(choice, axis=0)
        chosen = first[None, :, None] == jnp.arange(len(SPLITS), dtype=jnp.int32)[:, None, None]
        slot_now = jnp.sum(jnp.where(chosen, slot, 0), axis=0)
        steps_now = jnp.sum(jnp.where(chosen, steps, 0), axis=0)
        right_now = jnp.any(chosen & to_right, axis=0)
        wide, total = used[0], sum(used)
        stage = shard_blocks + 1
        moved = steps_now > 0
        begun = sum(
            jnp.where(steps_now > k + 1, n, 0) for k, n in enumerate(used)
        )
        at = stage + 2 * wide + jnp.where(right_now, 0, total) + begun + slot_now
        at = jnp.where(moved, at, jnp.arange(shard_blocks, dtype=jnp.int32)[None, :]).reshape(-1)
        of_nth = jnp.sum(jnp.where(nth, at[None, :] - shard_blocks, 0), axis=1)
        source = jnp.sum(jnp.where(row_of, of_nth[:, None], 0), axis=0) + shard_blocks
        spot = jnp.where(right_now, 0, wide) + slot_now
        spot = jnp.where(moved, spot, -1)
        spot = lax.dynamic_slice_in_dim(spot, me, 1)[0]
        hit = jnp.arange(2 * wide, dtype=jnp.int32)[:, None] == spot[None, :]
        pick = jnp.sum(jnp.where(hit, jnp.arange(shard_blocks, dtype=jnp.int32)[None, :], 0), axis=1)
        return ring(
            used, number + 1, seq, capacity, requests, own, done, pick, source, row_source
        )

    decode_cache, rows = lax.switch(
        tier, [functools.partial(deliver, number) for number in range(len(schedules))]
    )
    return (decode_cache, rows.reshape(requests, -1))


def solution(mesh):
    return jax.shard_map(
        functools.partial(
            per_device, mesh.shape["tp"], mesh.shape["sub"], mesh.shape["groups"], mesh.shape["seq"]
        ),
        mesh=mesh,
        in_specs=(
            P(("groups", "seq"), None, ("tp", "sub"), None),
            P("groups"),
            P("groups"),
            P("groups", None),
            P("groups", ("tp", "sub")),
            P("groups", None, ("tp", "sub")),
        ),
        out_specs=(P(("groups", "seq"), None, None, ("tp", "sub")), P("groups", ("tp", "sub"))),
        check_vma=False,
    )
```

```python
import functools

import jax
import jax.numpy as jnp
from jax import lax
from jax.experimental import pallas as pl
from jax.experimental.pallas import tpu as pltpu
from jax.sharding import PartitionSpec as P

HD = 128
BLOCK = 128
NEG_FLOOR = -1e30
MESH = pl.DeviceIdType.MESH
SPLITS = (13, 14, 15, 16, 17, 18)


def loads(steps_of_slot):
    return tuple(sum(c >= k for c in steps_of_slot) for k in range(1, max(steps_of_slot) + 1))


def tiers(shard_blocks, seq):
    half = seq // 2
    picks = [
        [18, 17, 15, 14, 12, 11, 9, 8, 6, 5, 3],
        [18, 17, 15, 14, 13, 12, 10, 9, 8, 6, 5, 4, 2],
    ]
    every = [half - i // 2 for i in range(shard_blocks)]
    return tuple((loads(p), shard_blocks // 2) for p in picks) + ((loads(every), shard_blocks),)


def exchange_kernel(tp, sub, groups, x_ref, tier_ref, own_ref, tiers_ref, sem, send_sem, recv_sem, tier_send, tier_recv):
    group = lax.axis_index("groups")
    parts = head_parts(tp, sub, 0, x_ref, own_ref, sem, send_sem, recv_sem)
    others = [{"groups": lax.rem(group + step, groups)} for step in range(1, groups)]
    barrier = pltpu.get_barrier_semaphore()
    for where in head_peers(tp, sub) + others:
        pl.semaphore_signal(barrier, inc=1, device_id=where, device_id_type=MESH)
    pl.semaphore_wait(barrier, tp * sub + groups - 2)
    for step, where in enumerate(others):
        parts.append(
            pltpu.make_async_remote_copy(
                src_ref=tier_ref,
                dst_ref=tiers_ref.at[group],
                send_sem=tier_send.at[step],
                recv_sem=tier_recv.at[step],
                device_id=where,
                device_id_type=MESH,
            )
        )
    for part in parts:
        part.start()
    tiers_ref[group] = tier_ref[...]
    for part in parts:
        part.wait()


def head_peers(tp, sub):
    me = lax.axis_index("tp") * sub + lax.axis_index("sub")
    others = [lax.rem(me + step, tp * sub) for step in range(1, tp * sub)]
    return [{"tp": other // sub, "sub": lax.rem(other, sub)} for other in others]


def head_parts(tp, sub, half, x_ref, own_ref, sem, send_sem, recv_sem):
    width = own_ref.shape[2]
    rows = x_ref.shape[2]
    me = lax.axis_index("tp") * sub + lax.axis_index("sub")
    mine = pl.ds(pl.multiple_of(me * rows, rows), rows)
    target = own_ref.at[:, mine, :]
    parts = [
        pltpu.make_async_copy(
            x_ref.at[:, half, :, pl.ds(pl.multiple_of(me * width, width), width)], target, sem
        )
    ]
    for step, where in enumerate(head_peers(tp, sub)):
        other = where["tp"] * sub + where["sub"]
        parts.append(
            pltpu.make_async_remote_copy(
                src_ref=x_ref.at[:, half, :, pl.ds(pl.multiple_of(other * width, width), width)],
                dst_ref=target,
                send_sem=send_sem.at[step],
                recv_sem=recv_sem.at[step],
                device_id=where,
                device_id_type=MESH,
            )
        )
    return parts


def exchange(prefill_kv, tier, tp, sub, groups):
    blocks, _, rows, columns = prefill_kv.shape
    count = tp * sub
    return pl.pallas_call(
        functools.partial(exchange_kernel, tp, sub, groups),
        out_shape=(
            jax.ShapeDtypeStruct((blocks, rows * count, columns // count), prefill_kv.dtype),
            jax.ShapeDtypeStruct((groups, 8, 128), jnp.int32),
        ),
        in_specs=[pl.BlockSpec(memory_space=pl.ANY), pl.BlockSpec(memory_space=pltpu.VMEM)],
        out_specs=[pl.BlockSpec(memory_space=pltpu.VMEM)] * 2,
        scratch_shapes=[
            pltpu.SemaphoreType.DMA,
            pltpu.SemaphoreType.DMA((count,)),
            pltpu.SemaphoreType.DMA((count,)),
            pltpu.SemaphoreType.DMA((groups,)),
            pltpu.SemaphoreType.DMA((groups,)),
        ],
        compiler_params=pltpu.CompilerParams(collective_id=0, has_side_effects=True),
    )(prefill_kv, jnp.broadcast_to(tier, (8, 128)))


def ring_kernel(
    used, slots, tp, sub, seq,
    x_ref, keys_ref, query_ref, new_ref, plan_ref, table_ref, cache_ref, rows_ref,
    klog, vlog, values, alog, states, came, sem, head_send, head_recv, send_sem, recv_sem, asend_sem, arecv_sem,
    state_send, state_recv,
):
    me = lax.axis_index("seq")

    def along(step):
        return {"seq": lax.rem(me + step + seq, seq)}

    blocks = keys_ref.shape[0]
    capacity, requests = cache_ref.shape[0], rows_ref.shape[0]
    group_size = query_ref.shape[1]
    wide, total = used[0], sum(used)
    starts = [sum(used[:k]) for k in range(len(used))]
    stage = blocks + 1
    base = (stage + 2 * wide, stage + 2 * wide + total)
    reach = (seq // 2, seq - 1 - seq // 2)
    logs = (klog, vlog)
    of_row, of_request, of_block = 2 * wide, 0, 2 * requests
    of_done = of_block + 3 * blocks

    def stage_half(log, own_ref):
        log[blocks] = jnp.zeros(log.shape[1:], log.dtype)

        def keep(i, carry):
            log[i] = own_ref[i]
            return carry

        lax.fori_loop(0, blocks, keep, 0)

        def pick(i, carry):
            log[stage + i] = own_ref[plan_ref[i]]
            return carry

        lax.fori_loop(0, 2 * wide, pick, 0)

    def block_copy(half, way, step, i):
        at = starts[step] + i
        source = stage + way * wide + i if step == 0 else base[way] + starts[step - 1] + i
        return pltpu.make_async_remote_copy(
            src_ref=logs[half].at[source],
            dst_ref=logs[half].at[base[way] + at],
            send_sem=send_sem.at[half, way],
            recv_sem=recv_sem.at[half, way, at],
            device_id=along((1, -1)[way]),
            device_id_type=MESH,
        )

    def forward(half, step):
        def body(i, carry):
            for way in range(2):
                if step > 0:
                    block_copy(half, way, step - 1, i).wait_recv()
                block_copy(half, way, step, i).start()
            return carry

        lax.fori_loop(0, used[step], body, 0)

    def land(half, step):
        beyond = used[step + 1] if step + 1 < len(used) else 0

        def body(i, carry):
            for way in range(2):
                block_copy(half, way, step, i).wait_recv()
            return carry

        lax.fori_loop(beyond, used[step], body, 0)

    def row_copy(way, step):
        at = way * reach[0] + step + 1
        source = 0 if step == 0 else at - 1
        return pltpu.make_async_remote_copy(
            src_ref=alog.at[pl.ds(source * slots, slots)],
            dst_ref=alog.at[pl.ds(at * slots, slots)],
            send_sem=asend_sem.at[at],
            recv_sem=arecv_sem.at[at],
            device_id=along((1, -1)[way]),
            device_id_type=MESH,
        )

    def state_copy(step):
        return pltpu.make_async_remote_copy(
            src_ref=states.at[blocks - 1],
            dst_ref=came.at[step],
            send_sem=state_send.at[step],
            recv_sem=state_recv.at[step],
            device_id=along(step + 1),
            device_id_type=MESH,
        )

    stage_half(klog, keys_ref)

    barrier = pltpu.get_barrier_semaphore()
    met = head_peers(tp, sub) + [along(step) for step in (1, -1, 2, -2)]
    for where in met:
        pl.semaphore_signal(barrier, inc=1, device_id=where, device_id_type=MESH)
    pl.semaphore_wait(barrier, len(met))

    parts = head_parts(tp, sub, 1, x_ref, values, sem, head_send, head_recv)
    for part in parts:
        part.start()
    forward(0, 0)

    scale = HD ** (-0.5)
    token = lax.broadcasted_iota(jnp.int32, (group_size, BLOCK), 1)
    weights, peaks, sums = [], [], []
    for b in range(blocks):
        query = query_ref[table_ref[of_block + b]]
        score = scale * lax.dot_general(
            query, keys_ref[b], (((1,), (1,)), ((), ())), preferred_element_type=jnp.float32
        )
        score = jnp.where(token < table_ref[of_block + blocks + b], score, NEG_FLOOR)
        peak = jnp.max(score, axis=1, keepdims=True)
        weight = jnp.exp(score - peak).astype(jnp.bfloat16)
        weights.append(weight)
        peaks.append(jnp.broadcast_to(peak, (group_size, HD)))
        sums.append(
            jnp.broadcast_to(
                jnp.sum(weight.astype(jnp.float32), axis=1, keepdims=True), (group_size, HD)
            )
        )

    def merge(first, second):
        top = jnp.maximum(first[0], second[0])
        one, two = jnp.exp(first[0] - top), jnp.exp(second[0] - top)
        return (top, one * first[1] + two * second[1], one * first[2] + two * second[2])

    def attend():
        state = None
        for b in range(blocks):
            partial = jnp.dot(weights[b], values[b], preferred_element_type=jnp.float32)
            fresh = (peaks[b], sums[b], partial)
            if state is not None:
                begins = table_ref[of_block + 2 * blocks + b] > 0
                joined = merge(state, fresh)
                fresh = tuple(jnp.where(begins, f, j) for f, j in zip(fresh, joined))
            state = fresh
            for part in range(3):
                states[b, part] = state[part]

    def answer(j, carry):
        request = table_ref[of_done + j]
        block = table_ref[of_done + blocks + j]
        state = tuple(states[block, part] for part in range(3))
        for back in range(2):
            enters = table_ref[of_done + (2 + back) * blocks + j] > 0
            joined = merge(state, tuple(came[back, part] for part in range(3)))
            state = tuple(jnp.where(enters, f, s) for f, s in zip(joined, state))
        new = new_ref[request]
        own = scale * jnp.sum(
            query_ref[request].astype(jnp.float32) * new[0:1], axis=1, keepdims=True
        )
        own = jnp.broadcast_to(own, (group_size, HD))
        ones = jnp.ones((group_size, HD), jnp.float32)
        _, denom, numer = merge(state, (own, ones, jnp.broadcast_to(new[1:2], (group_size, HD))))
        alog[j] = (numer / denom).astype(alog.dtype)
        return carry

    lag = 3
    for turn in range(max(len(used) + 1, reach[0] + lag)):
        if 0 < turn < len(used):
            forward(0, turn)
        if turn == 1:
            for part in parts:
                part.wait()
            stage_half(vlog, values)
        if 0 < turn <= len(used):
            forward(1, turn - 1)
        if turn == 1:
            attend()
        if turn == 2:
            for step in range(2):
                state_copy(step).start()
        if turn == lag:
            for step in range(2):
                state_copy(step).wait()
            lax.fori_loop(0, slots, answer, 0)
        for way in range(2):
            if 0 <= turn - lag < reach[way]:
                if turn > lag:
                    row_copy(way, turn - lag - 1).wait_recv()
                row_copy(way, turn - lag).start()

    for half in range(2):
        for step in range(len(used)):
            land(half, step)
    for way in range(2):
        row_copy(way, reach[way] - 1).wait_recv()
        for step in range(reach[way]):
            row_copy(way, step).wait_send()
        for half in range(2):
            every = logs[half].at[pl.ds(base[way], total)]
            pltpu.make_async_remote_copy(
                src_ref=every,
                dst_ref=every,
                send_sem=send_sem.at[half, way],
                recv_sem=recv_sem.at[half, way, 0],
                device_id=along((1, -1)[way]),
                device_id_type=MESH,
            ).wait_send()

    def place(c, carry):
        source = plan_ref[of_row + c]
        cache_ref[c, 0] = klog[source]
        cache_ref[c, 1] = vlog[source]
        return carry

    lax.fori_loop(0, capacity, place, 0)

    def collect(r, carry):
        rows_ref[r] = alog[table_ref[of_request + r] * slots + table_ref[of_request + requests + r]]
        return carry

    lax.fori_loop(0, requests, collect, 0)


def ring(used, slots, number, tp, sub, seq, capacity, prefill_kv, keys, queries, new_kv, plan, table):
    blocks = keys.shape[0]
    wide, total = used[0], sum(used)
    requests, group_size = queries.shape[:2]
    count = tp * sub
    vmem = pl.BlockSpec(memory_space=pltpu.VMEM)
    smem = pl.BlockSpec(memory_space=pltpu.SMEM)
    log = pltpu.VMEM((blocks + 1 + 2 * wide + 2 * total,) + keys.shape[1:], keys.dtype)
    return pl.pallas_call(
        functools.partial(ring_kernel, used, slots, tp, sub, seq),
        out_shape=(
            jax.ShapeDtypeStruct((capacity, 2) + keys.shape[1:], keys.dtype),
            jax.ShapeDtypeStruct((requests, group_size, HD), jnp.bfloat16),
        ),
        in_specs=[pl.BlockSpec(memory_space=pl.ANY), vmem, vmem, vmem, smem, smem],
        out_specs=(vmem, vmem),
        scratch_shapes=[
            log,
            log,
            pltpu.VMEM(keys.shape, keys.dtype),
            pltpu.VMEM((seq * slots, group_size, HD), jnp.bfloat16),
            pltpu.VMEM((blocks, 3, group_size, HD), jnp.float32),
            pltpu.VMEM((2, 3, group_size, HD), jnp.float32),
            pltpu.SemaphoreType.DMA,
            pltpu.SemaphoreType.DMA((count,)),
            pltpu.SemaphoreType.DMA((count,)),
            pltpu.SemaphoreType.DMA((2, 2)),
            pltpu.SemaphoreType.DMA((2, 2, total)),
            pltpu.SemaphoreType.DMA((seq,)),
            pltpu.SemaphoreType.DMA((seq,)),
            pltpu.SemaphoreType.DMA((2,)),
            pltpu.SemaphoreType.DMA((2,)),
        ],
        compiler_params=pltpu.CompilerParams(
            collective_id=number, has_side_effects=True, vmem_limit_bytes=60 << 20
        ),
    )(prefill_kv, keys, queries, new_kv, plan, table)


def travel(used, slot):
    return sum((slot < n).astype(jnp.int32) for n in used)


def lookup(hot, values):
    return jnp.sum(jnp.where(hot, values[None, :], 0), axis=1)


def per_device(tp, sub, groups, seq, prefill_kv, prompt_lengths, block_owner, slot_order, queries, new_kv):
    me = lax.axis_index("seq")
    shard_blocks = prefill_kv.shape[0]
    capacity = slot_order.shape[1]
    requests = prompt_lengths.shape[0]
    schedules = tiers(shard_blocks, seq)
    local = jnp.arange(shard_blocks, dtype=jnp.int32)
    ids = jnp.arange(requests, dtype=jnp.int32)

    counts = (prompt_lengths + BLOCK - 1) // BLOCK
    block_ends = jnp.sum(jnp.where(ids[None, :] <= ids[:, None], counts[None, :], 0), axis=1)
    block_starts = block_ends - counts
    last_shard = (block_ends - 1) // shard_blocks
    alike = last_shard[:, None] == last_shard[None, :]
    place = jnp.sum((alike & (ids[None, :] < ids[:, None])).astype(jnp.int32), axis=1)
    most_done = jnp.max(place) + 1

    owners = block_owner.reshape(seq, shard_blocks)
    shards = jnp.arange(seq, dtype=jnp.int32)
    ahead = lax.rem(owners - shards[:, None] + seq, seq)
    key = ahead * shard_blocks + local[None, :]
    order = jnp.sum((key[:, None, :] < key[:, :, None]).astype(jnp.int32), axis=2)
    split = jnp.array(SPLITS, jnp.int32)
    to_right = ahead[None] <= split[:, None, None]
    rightward = jnp.sum(to_right.astype(jnp.int32), axis=2, keepdims=True)
    slot = jnp.where(to_right, rightward - 1 - order[None], order[None] - rightward)
    steps = jnp.where(to_right, ahead[None], seq - ahead[None])
    steps = jnp.where(ahead[None] == 0, 0, steps)
    fits = jnp.stack([jnp.all(steps <= travel(used, slot), axis=2) for used, _ in schedules])
    shard_fits = jnp.any(fits, axis=1)
    tier_fits = jnp.all(shard_fits, axis=1) & jnp.stack([most_done <= slots for _, slots in schedules])
    own_tier = jnp.minimum(jnp.sum((~tier_fits).astype(jnp.int32)), len(schedules) - 1)

    keys, agreed = exchange(prefill_kv, own_tier, tp, sub, groups)
    tier = jnp.max(agreed)

    low = me * shard_blocks
    behind = lax.rem(me - last_shard + seq, seq)
    half = seq // 2
    came_at = jnp.where(behind <= half, behind, half + seq - behind)
    blocks_at = low + local
    member = (blocks_at[:, None] >= block_starts[None, :]) & (blocks_at[:, None] < block_ends[None, :])
    block_request = lookup(member, ids)
    valid = jnp.clip(
        lookup(member, prompt_lengths) - (blocks_at - lookup(member, block_starts)) * BLOCK, 0, BLOCK
    )
    begins = jnp.any(blocks_at[:, None] == block_starts[None, :], axis=1).astype(jnp.int32)
    first_done = jnp.sum((last_shard < me).astype(jnp.int32))
    done = jnp.minimum(first_done + local, requests - 1)
    is_done = done[:, None] == ids[None, :]
    done_block = jnp.clip(lookup(is_done, block_ends) - 1 - low, 0, shard_blocks - 1)
    done_start = lookup(is_done, block_starts)
    enters = [(done_start < low - back * shard_blocks).astype(jnp.int32) for back in range(2)]
    table = jnp.concatenate([came_at, place, block_request, valid, begins, done, done_block] + enters)

    mine = block_owner == me
    rank = jnp.cumsum(mine.astype(jnp.int32)) - 1
    own_slots = lax.dynamic_slice_in_dim(slot_order, me, 1)[0]
    nth = mine[None, :] & (rank[None, :] == jnp.arange(capacity, dtype=jnp.int32)[:, None])
    row_of = own_slots[:, None] == jnp.arange(capacity, dtype=jnp.int32)[None, :]

    query_rows = queries.reshape(requests, -1, HD)
    new_rows = new_kv.astype(jnp.float32)

    def deliver(number):
        used, slots = schedules[number]
        choice = fits[number]
        first = jnp.argmax(choice, axis=0)
        chosen = first[None, :, None] == jnp.arange(len(SPLITS), dtype=jnp.int32)[:, None, None]
        slot_now = jnp.sum(jnp.where(chosen, slot, 0), axis=0)
        steps_now = jnp.sum(jnp.where(chosen, steps, 0), axis=0)
        right_now = jnp.any(chosen & to_right, axis=0)
        wide, total = used[0], sum(used)
        stage = shard_blocks + 1
        moved = steps_now > 0
        begun = sum(
            jnp.where(steps_now > k + 1, n, 0) for k, n in enumerate(used)
        )
        at = stage + 2 * wide + jnp.where(right_now, 0, total) + begun + slot_now
        at = jnp.where(moved, at, local[None, :]).reshape(-1)
        of_nth = jnp.sum(jnp.where(nth, at[None, :] - shard_blocks, 0), axis=1)
        source = jnp.sum(jnp.where(row_of, of_nth[:, None], 0), axis=0) + shard_blocks
        spot = jnp.where(right_now, 0, wide) + slot_now
        spot = jnp.where(moved, spot, -1)
        spot = lax.dynamic_slice_in_dim(spot, me, 1)[0]
        hit = jnp.arange(2 * wide, dtype=jnp.int32)[:, None] == spot[None, :]
        pick = jnp.sum(jnp.where(hit, local[None, :], 0), axis=1)
        plan = jnp.concatenate([pick, source])
        return ring(
            used, slots, number + 1, tp, sub, seq, capacity,
            prefill_kv, keys, query_rows, new_rows, plan, table,
        )

    decode_cache, rows = lax.switch(
        tier, [functools.partial(deliver, number) for number in range(len(schedules))]
    )
    return (decode_cache, rows.reshape(requests, -1))


def solution(mesh):
    return jax.shard_map(
        functools.partial(
            per_device, mesh.shape["tp"], mesh.shape["sub"], mesh.shape["groups"], mesh.shape["seq"]
        ),
        mesh=mesh,
        in_specs=(
            P(("groups", "seq"), None, ("tp", "sub"), None),
            P("groups"),
            P("groups"),
            P("groups", None),
            P("groups", ("tp", "sub")),
            P("groups", None, ("tp", "sub")),
        ),
        out_specs=(P(("groups", "seq"), None, None, ("tp", "sub")), P("groups", ("tp", "sub"))),
        check_vma=False,
    )
```

```python
import functools

import jax
import jax.numpy as jnp
from jax import lax
from jax.experimental import pallas as pl
from jax.experimental.pallas import tpu as pltpu
from jax.sharding import PartitionSpec as P

HD = 128
BLOCK = 128
NEG_FLOOR = -1e30
MESH = pl.DeviceIdType.MESH
SPLITS = (16, 15, 17, 14, 18, 13, 19, 12)
LANES = 128


def loads(steps_of_slot):
    return tuple(sum(c >= k for c in steps_of_slot) for k in range(1, max(steps_of_slot) + 1))


def tiers(shard_blocks, seq):
    half = seq // 2
    picks = [
        [18, 17, 16, 14, 12, 11, 9, 8, 6, 4, 3, 1],
        [18, 17, 16, 14, 13, 11, 10, 9, 8, 6, 5, 2, 1],
    ]
    every = [half - i // 2 for i in range(shard_blocks)]
    return tuple((loads(p), shard_blocks // 2) for p in picks) + ((loads(every), shard_blocks),)


def count_of(mask, axis):
    return jnp.sum(mask.astype(jnp.int32), axis=axis, keepdims=True)


def total_of(mask, values, axis):
    return jnp.sum(jnp.where(mask, values, 0), axis=axis, keepdims=True)


def request_plan(blocks, seq, requests, length_ref, table_ref):
    me = lax.axis_index("seq")
    low = me * blocks
    down = lax.broadcasted_iota(jnp.int32, (LANES, LANES), 0)
    across = lax.broadcasted_iota(jnp.int32, (LANES, LANES), 1)
    lane = lax.broadcasted_iota(jnp.int32, (1, LANES), 1)
    lengths = jnp.broadcast_to(length_ref[0:1], (LANES, LANES))
    length = total_of(down == across, lengths, 1)
    counts = (lengths + BLOCK - 1) // BLOCK
    ends = total_of(across <= down, counts, 1)
    starts = total_of(across < down, counts, 1)
    ends_row = total_of(down == across, jnp.broadcast_to(ends, (LANES, LANES)), 0)
    shard, shard_row = (ends - 1) // blocks, (ends_row - 1) // blocks
    real = down < requests
    place = count_of(real & (down < across) & (shard == shard_row), 0)
    behind = me - shard_row
    behind = jnp.where(behind < 0, behind + seq, behind)
    half = seq // 2
    came_at = jnp.where(behind <= half, behind, half + seq - behind)
    block = low + lane
    member = (block >= starts) & (block < ends)
    request = jnp.minimum(count_of(real & (ends <= block), 0), requests - 1)
    valid = total_of(member, jnp.clip(length - (block - starts) * BLOCK, 0, BLOCK), 0)
    begins = count_of(real & (block == starts), 0)
    done = jnp.minimum(count_of(real & (shard < me), 0) + lane, requests - 1)
    done_block = jnp.clip(total_of(down == done, ends, 0) - 1 - low, 0, blocks - 1)
    done_start = total_of(down == done, starts, 0)
    enters = [(done_start < low - back * blocks).astype(jnp.int32) for back in range(2)]
    for row, values in enumerate([came_at, place, request, valid, begins, done, done_block] + enters):
        table_ref[row : row + 1] = values
    return jnp.max(jnp.where(lane < requests, place, 0), axis=1, keepdims=True) + 1


def ring_plan(schedules, seq, most_done, owner_ref, order_ref, plan_ref, found_ref):
    blocks = owner_ref.shape[0]
    capacity = order_ref.shape[1]
    shape = (blocks, LANES)
    me = lax.axis_index("seq")
    down = lax.broadcasted_iota(jnp.int32, shape, 0)
    across = lax.broadcasted_iota(jnp.int32, shape, 1)
    lane = lax.broadcasted_iota(jnp.int32, (1, LANES), 1)
    shards = across < seq
    owner = owner_ref[...]
    ahead = owner - across
    ahead = jnp.where(shards, jnp.where(ahead < 0, ahead + seq, ahead), 0)
    key = ahead * blocks + down
    order = jnp.zeros(shape, jnp.int32)
    for b in range(blocks):
        order = order + (key[b : b + 1] < key).astype(jnp.int32)
    moved = ahead > 0

    fitted = [None] * len(schedules)
    for split in SPLITS:
        right = ahead <= split
        rightward = count_of(right, 0)
        slot = jnp.where(right, rightward - 1 - order, order - rightward)
        steps = jnp.where(moved, jnp.where(right, ahead, seq - ahead), 0)
        for number, (used, _) in enumerate(schedules):
            excess = jnp.max(steps - travel(used, slot), axis=0, keepdims=True)
            fit = jnp.broadcast_to((excess <= 0).astype(jnp.int32), shape)
            now = (fit, slot, steps, right.astype(jnp.int32))
            if fitted[number] is None:
                fitted[number] = now
            else:
                before = fitted[number][0] > 0
                fitted[number] = tuple(jnp.where(before, f, n) for f, n in zip(fitted[number], now))

    mine = (owner == me) & shards
    hot = mine.astype(jnp.float32)
    earlier = jnp.zeros(shape, jnp.float32)
    for b in range(blocks - 1):
        earlier = earlier + jnp.where(down > b, hot[b : b + 1], 0.0)
    each = jnp.broadcast_to(jnp.sum(hot, axis=0, keepdims=True), shape)
    ahead_of = lax.broadcasted_iota(jnp.int32, (LANES, LANES), 0) < lax.broadcasted_iota(
        jnp.int32, (LANES, LANES), 1
    )
    prior = jnp.dot(
        each.astype(jnp.bfloat16),
        ahead_of.astype(jnp.float32).astype(jnp.bfloat16),
        preferred_element_type=jnp.float32,
    )
    rank = (earlier + prior).astype(jnp.int32)
    row = jnp.full(shape, -1, jnp.int32)
    for k in range(capacity):
        row = jnp.where(mine & (rank == k), order_ref[me, k], row)

    tier = jnp.zeros((1, 1), jnp.int32)
    for number, (used, slots) in enumerate(schedules):
        fit, slot, steps, right = fitted[number]
        fits = jnp.min(fit[0:1], axis=1, keepdims=True) * (most_done <= slots).astype(jnp.int32)
        if number < len(schedules) - 1:
            tier = tier + 1 - fits
        wide, total = used[0], sum(used)
        begun = sum(jnp.where(steps > k + 1, n, 0) for k, n in enumerate(used))
        at = blocks + 1 + 2 * wide + jnp.where(right > 0, 0, total) + begun + slot
        at = jnp.where(moved, at, down)
        for c in range(capacity):
            found_ref[c : c + 1] = total_of(row == c, at + 1, 0)
        found = jnp.sum(found_ref[...], axis=1, keepdims=True)
        diagonal = lax.broadcasted_iota(jnp.int32, found_ref.shape, 0) == lax.broadcasted_iota(
            jnp.int32, found_ref.shape, 1
        )
        source = total_of(diagonal, jnp.broadcast_to(found, found_ref.shape), 0)
        spot = jnp.where(moved, jnp.where(right > 0, 0, wide) + slot, -1)
        spot = total_of(across == me, spot + 1, 1) - 1
        plan_ref[2 * number : 2 * number + 1] = total_of(spot == across, down, 0)
        plan_ref[2 * number + 1 : 2 * number + 2] = jnp.where(source > 0, source - 1, blocks)
    return tier


def exchange_kernel(
    tp, sub, groups, seq, requests, schedules,
    x_ref, owner_ref, length_ref, order_ref, own_ref, tier_ref, plan_ref, table_ref,
    found, tiers, sem, send_sem, recv_sem, tier_send, tier_recv,
):
    group = lax.axis_index("groups")
    parts = head_parts(tp, sub, 0, x_ref, own_ref, sem, send_sem, recv_sem)
    others = [{"groups": lax.rem(group + step, groups)} for step in range(1, groups)]
    barrier = pltpu.get_barrier_semaphore()
    for where in head_peers(tp, sub) + others:
        pl.semaphore_signal(barrier, inc=1, device_id=where, device_id_type=MESH)
    pl.semaphore_wait(barrier, tp * sub + groups - 2)
    for part in parts:
        part.start()
    blocks = x_ref.shape[0]
    most_done = request_plan(blocks, seq, requests, length_ref, table_ref)
    tier = ring_plan(schedules, seq, most_done, owner_ref, order_ref, plan_ref, found)
    tiers[0] = jnp.broadcast_to(tier, tiers.shape[1:])
    told = [
        pltpu.make_async_remote_copy(
            src_ref=tiers.at[0],
            dst_ref=tiers.at[step + 1],
            send_sem=tier_send.at[step],
            recv_sem=tier_recv.at[step],
            device_id=where,
            device_id_type=MESH,
        )
        for step, where in enumerate(others)
    ]
    for part in told:
        part.start()
    for part in told + parts:
        part.wait()
    agreed = tiers[0]
    for step in range(len(others)):
        agreed = jnp.maximum(agreed, tiers[step + 1])
    tier_ref[...] = agreed


def head_peers(tp, sub):
    me = lax.axis_index("tp") * sub + lax.axis_index("sub")
    others = [lax.rem(me + step, tp * sub) for step in range(1, tp * sub)]
    return [{"tp": other // sub, "sub": lax.rem(other, sub)} for other in others]


def head_parts(tp, sub, half, x_ref, own_ref, sem, send_sem, recv_sem):
    width = own_ref.shape[2]
    rows = x_ref.shape[2]
    me = lax.axis_index("tp") * sub + lax.axis_index("sub")
    mine = pl.ds(pl.multiple_of(me * rows, rows), rows)
    target = own_ref.at[:, mine, :]
    parts = [
        pltpu.make_async_copy(
            x_ref.at[:, half, :, pl.ds(pl.multiple_of(me * width, width), width)], target, sem
        )
    ]
    for step, where in enumerate(head_peers(tp, sub)):
        other = where["tp"] * sub + where["sub"]
        parts.append(
            pltpu.make_async_remote_copy(
                src_ref=x_ref.at[:, half, :, pl.ds(pl.multiple_of(other * width, width), width)],
                dst_ref=target,
                send_sem=send_sem.at[step],
                recv_sem=recv_sem.at[step],
                device_id=where,
                device_id_type=MESH,
            )
        )
    return parts


def exchange(prefill_kv, owners, lengths, slot_order, requests, schedules, tp, sub, groups, seq):
    blocks, _, rows, columns = prefill_kv.shape
    capacity = slot_order.shape[1]
    count = tp * sub
    vmem = pl.BlockSpec(memory_space=pltpu.VMEM)
    return pl.pallas_call(
        functools.partial(exchange_kernel, tp, sub, groups, seq, requests, schedules),
        out_shape=(
            jax.ShapeDtypeStruct((blocks, rows * count, columns // count), prefill_kv.dtype),
            jax.ShapeDtypeStruct((8, LANES), jnp.int32),
            jax.ShapeDtypeStruct((8, LANES), jnp.int32),
            jax.ShapeDtypeStruct((16, LANES), jnp.int32),
        ),
        in_specs=[pl.BlockSpec(memory_space=pl.ANY), vmem, vmem, pl.BlockSpec(memory_space=pltpu.SMEM)],
        out_specs=[vmem] * 4,
        scratch_shapes=[
            pltpu.VMEM((capacity, LANES), jnp.int32),
            pltpu.VMEM((groups, 8, LANES), jnp.int32),
            pltpu.SemaphoreType.DMA,
            pltpu.SemaphoreType.DMA((count,)),
            pltpu.SemaphoreType.DMA((count,)),
            pltpu.SemaphoreType.DMA((groups,)),
            pltpu.SemaphoreType.DMA((groups,)),
        ],
        compiler_params=pltpu.CompilerParams(collective_id=0, has_side_effects=True),
    )(prefill_kv, owners, lengths, slot_order)


def ring_kernel(
    used, slots, number, tp, sub, seq,
    x_ref, keys_ref, query_ref, new_ref, plan_ref, table_ref, cache_ref, rows_ref,
    klog, vlog, values, alog, states, came, sem, head_send, head_recv, send_sem, recv_sem, asend_sem, arecv_sem,
    state_send, state_recv,
):
    me = lax.axis_index("seq")

    def along(step):
        return {"seq": lax.rem(me + step + seq, seq)}

    blocks = keys_ref.shape[0]
    capacity, requests = cache_ref.shape[0], rows_ref.shape[0]
    group_size = query_ref.shape[1]
    wide, total = used[0], sum(used)
    starts = [sum(used[:k]) for k in range(len(used))]
    stage = blocks + 1
    base = (stage + 2 * wide, stage + 2 * wide + total)
    reach = (seq // 2, seq - 1 - seq // 2)
    logs = (klog, vlog)

    def stage_half(log, own_ref):
        log[blocks] = jnp.zeros(log.shape[1:], log.dtype)

        def keep(i, carry):
            log[i] = own_ref[i]
            return carry

        lax.fori_loop(0, blocks, keep, 0)

        def pick(i, carry):
            log[stage + i] = own_ref[plan_ref[2 * number, i]]
            return carry

        lax.fori_loop(0, 2 * wide, pick, 0)

    def block_copy(half, way, step, i):
        at = starts[step] + i
        source = stage + way * wide + i if step == 0 else base[way] + starts[step - 1] + i
        return pltpu.make_async_remote_copy(
            src_ref=logs[half].at[source],
            dst_ref=logs[half].at[base[way] + at],
            send_sem=send_sem.at[half, way],
            recv_sem=recv_sem.at[half, way, at],
            device_id=along((1, -1)[way]),
            device_id_type=MESH,
        )

    def forward(half, step):
        def body(i, carry):
            for way in range(2):
                if step > 0:
                    block_copy(half, way, step - 1, i).wait_recv()
                block_copy(half, way, step, i).start()
            return carry

        lax.fori_loop(0, used[step], body, 0)

    def land(half, step):
        beyond = used[step + 1] if step + 1 < len(used) else 0

        def body(i, carry):
            for way in range(2):
                block_copy(half, way, step, i).wait_recv()
            return carry

        lax.fori_loop(beyond, used[step], body, 0)

    def row_copy(way, step):
        at = way * reach[0] + step + 1
        source = 0 if step == 0 else at - 1
        return pltpu.make_async_remote_copy(
            src_ref=alog.at[pl.ds(source * slots, slots)],
            dst_ref=alog.at[pl.ds(at * slots, slots)],
            send_sem=asend_sem.at[at],
            recv_sem=arecv_sem.at[at],
            device_id=along((1, -1)[way]),
            device_id_type=MESH,
        )

    def state_copy(step):
        return pltpu.make_async_remote_copy(
            src_ref=states.at[blocks - 1],
            dst_ref=came.at[step],
            send_sem=state_send.at[step],
            recv_sem=state_recv.at[step],
            device_id=along(step + 1),
            device_id_type=MESH,
        )

    stage_half(klog, keys_ref)

    barrier = pltpu.get_barrier_semaphore()
    met = head_peers(tp, sub) + [along(step) for step in (1, -1, 2, -2)]
    for where in met:
        pl.semaphore_signal(barrier, inc=1, device_id=where, device_id_type=MESH)
    pl.semaphore_wait(barrier, len(met))

    parts = head_parts(tp, sub, 1, x_ref, values, sem, head_send, head_recv)
    for part in parts:
        part.start()
    forward(0, 0)

    scale = HD ** (-0.5)
    token = lax.broadcasted_iota(jnp.int32, (group_size, BLOCK), 1)
    weights, peaks, sums = [], [], []
    for b in range(blocks):
        query = query_ref[table_ref[2, b]]
        score = scale * lax.dot_general(
            query, keys_ref[b], (((1,), (1,)), ((), ())), preferred_element_type=jnp.float32
        )
        score = jnp.where(token < table_ref[3, b], score, NEG_FLOOR)
        peak = jnp.max(score, axis=1, keepdims=True)
        weight = jnp.exp(score - peak).astype(jnp.bfloat16)
        weights.append(weight)
        peaks.append(jnp.broadcast_to(peak, (group_size, HD)))
        sums.append(
            jnp.broadcast_to(
                jnp.sum(weight.astype(jnp.float32), axis=1, keepdims=True), (group_size, HD)
            )
        )

    def merge(first, second):
        top = jnp.maximum(first[0], second[0])
        one, two = jnp.exp(first[0] - top), jnp.exp(second[0] - top)
        return (top, one * first[1] + two * second[1], one * first[2] + two * second[2])

    def attend():
        state = None
        for b in range(blocks):
            partial = jnp.dot(weights[b], values[b], preferred_element_type=jnp.float32)
            fresh = (peaks[b], sums[b], partial)
            if state is not None:
                begins = table_ref[4, b] > 0
                joined = merge(state, fresh)
                fresh = tuple(jnp.where(begins, f, j) for f, j in zip(fresh, joined))
            state = fresh
            for part in range(3):
                states[b, part] = state[part]

    def answer(j, carry):
        request = table_ref[5, j]
        block = table_ref[6, j]
        state = tuple(states[block, part] for part in range(3))
        for back in range(2):
            enters = table_ref[7 + back, j] > 0
            joined = merge(state, tuple(came[back, part] for part in range(3)))
            state = tuple(jnp.where(enters, f, s) for f, s in zip(joined, state))
        new = new_ref[request]
        own = scale * jnp.sum(
            query_ref[request].astype(jnp.float32) * new[0:1], axis=1, keepdims=True
        )
        own = jnp.broadcast_to(own, (group_size, HD))
        ones = jnp.ones((group_size, HD), jnp.float32)
        _, denom, numer = merge(state, (own, ones, jnp.broadcast_to(new[1:2], (group_size, HD))))
        alog[j] = (numer / denom).astype(alog.dtype)
        return carry

    lag = 3
    for turn in range(max(len(used) + 1, reach[0] + lag)):
        if 0 < turn < len(used):
            forward(0, turn)
        if turn == 1:
            for part in parts:
                part.wait()
            stage_half(vlog, values)
        if 0 < turn <= len(used):
            forward(1, turn - 1)
        if turn == 1:
            attend()
        if turn == 2:
            for step in range(2):
                state_copy(step).start()
        if turn == lag:
            for step in range(2):
                state_copy(step).wait()
            lax.fori_loop(0, slots, answer, 0)
        for way in range(2):
            if 0 <= turn - lag < reach[way]:
                if turn > lag:
                    row_copy(way, turn - lag - 1).wait_recv()
                row_copy(way, turn - lag).start()

    for half in range(2):
        for step in range(len(used)):
            land(half, step)
    for way in range(2):
        row_copy(way, reach[way] - 1).wait_recv()
        for step in range(reach[way]):
            row_copy(way, step).wait_send()
        for half in range(2):
            every = logs[half].at[pl.ds(base[way], total)]
            pltpu.make_async_remote_copy(
                src_ref=every,
                dst_ref=every,
                send_sem=send_sem.at[half, way],
                recv_sem=recv_sem.at[half, way, 0],
                device_id=along((1, -1)[way]),
                device_id_type=MESH,
            ).wait_send()

    def place(c, carry):
        source = plan_ref[2 * number + 1, c]
        cache_ref[c, 0] = klog[source]
        cache_ref[c, 1] = vlog[source]
        return carry

    lax.fori_loop(0, capacity, place, 0)

    def collect(r, carry):
        rows_ref[r] = alog[table_ref[0, r] * slots + table_ref[1, r]]
        return carry

    lax.fori_loop(0, requests, collect, 0)


def ring(used, slots, number, tp, sub, seq, capacity, prefill_kv, keys, queries, new_kv, plan, table):
    blocks = keys.shape[0]
    wide, total = used[0], sum(used)
    requests, group_size = queries.shape[:2]
    count = tp * sub
    vmem = pl.BlockSpec(memory_space=pltpu.VMEM)
    smem = pl.BlockSpec(memory_space=pltpu.SMEM)
    log = pltpu.VMEM((blocks + 1 + 2 * wide + 2 * total,) + keys.shape[1:], keys.dtype)
    return pl.pallas_call(
        functools.partial(ring_kernel, used, slots, number, tp, sub, seq),
        out_shape=(
            jax.ShapeDtypeStruct((capacity, 2) + keys.shape[1:], keys.dtype),
            jax.ShapeDtypeStruct((requests, group_size, HD), jnp.bfloat16),
        ),
        in_specs=[pl.BlockSpec(memory_space=pl.ANY), vmem, vmem, vmem, smem, smem],
        out_specs=(vmem, vmem),
        scratch_shapes=[
            log,
            log,
            pltpu.VMEM(keys.shape, keys.dtype),
            pltpu.VMEM((seq * slots, group_size, HD), jnp.bfloat16),
            pltpu.VMEM((blocks, 3, group_size, HD), jnp.float32),
            pltpu.VMEM((2, 3, group_size, HD), jnp.float32),
            pltpu.SemaphoreType.DMA,
            pltpu.SemaphoreType.DMA((count,)),
            pltpu.SemaphoreType.DMA((count,)),
            pltpu.SemaphoreType.DMA((2, 2)),
            pltpu.SemaphoreType.DMA((2, 2, total)),
            pltpu.SemaphoreType.DMA((seq,)),
            pltpu.SemaphoreType.DMA((seq,)),
            pltpu.SemaphoreType.DMA((2,)),
            pltpu.SemaphoreType.DMA((2,)),
        ],
        compiler_params=pltpu.CompilerParams(
            collective_id=number + 1, has_side_effects=True, vmem_limit_bytes=60 << 20
        ),
    )(prefill_kv, keys, queries, new_kv, plan, table)


def travel(used, slot):
    return sum((slot < n).astype(jnp.int32) for n in used)


def per_device(tp, sub, groups, seq, prefill_kv, prompt_lengths, block_owner, slot_order, queries, new_kv):
    shard_blocks = prefill_kv.shape[0]
    capacity = slot_order.shape[1]
    requests = prompt_lengths.shape[0]
    schedules = tiers(shard_blocks, seq)
    owners = jnp.pad(block_owner.reshape(seq, shard_blocks).T, ((0, 0), (0, LANES - seq)))
    lengths = jnp.broadcast_to(jnp.pad(prompt_lengths, (0, LANES - requests))[None], (8, LANES))
    keys, agreed, plan, table = exchange(
        prefill_kv, owners, lengths, slot_order, requests, schedules, tp, sub, groups, seq
    )
    query_rows = queries.reshape(requests, -1, HD)
    new_rows = new_kv.astype(jnp.float32)

    def deliver(number):
        used, slots = schedules[number]
        return ring(
            used, slots, number, tp, sub, seq, capacity,
            prefill_kv, keys, query_rows, new_rows, plan, table,
        )

    decode_cache, rows = lax.switch(
        agreed[0, 0], [functools.partial(deliver, number) for number in range(len(schedules))]
    )
    return (decode_cache, rows.reshape(requests, -1))


def solution(mesh):
    return jax.shard_map(
        functools.partial(
            per_device, mesh.shape["tp"], mesh.shape["sub"], mesh.shape["groups"], mesh.shape["seq"]
        ),
        mesh=mesh,
        in_specs=(
            P(("groups", "seq"), None, ("tp", "sub"), None),
            P("groups"),
            P("groups"),
            P("groups", None),
            P("groups", ("tp", "sub")),
            P("groups", None, ("tp", "sub")),
        ),
        out_specs=(P(("groups", "seq"), None, None, ("tp", "sub")), P("groups", ("tp", "sub"))),
        check_vma=False,
    )
```

```python
import functools

import jax
import jax.numpy as jnp
from jax import lax
from jax.experimental import pallas as pl
from jax.experimental.pallas import tpu as pltpu
from jax.sharding import PartitionSpec as P

HD = 128
BLOCK = 128
NEG_FLOOR = -1e30
MESH = pl.DeviceIdType.MESH
SPLITS = (16, 15, 17, 14, 18, 13, 19, 12)
LANES = 128


def loads(steps_of_slot):
    return tuple(sum(c >= k for c in steps_of_slot) for k in range(1, max(steps_of_slot) + 1))


def tiers(shard_blocks, seq):
    half = seq // 2
    picks = [
        [18, 17, 16, 14, 12, 11, 9, 8, 6, 4, 3, 1],
        [18, 17, 16, 14, 13, 11, 10, 9, 8, 6, 5, 2, 1],
    ]
    every = [half - i // 2 for i in range(shard_blocks)]
    return tuple((loads(p), shard_blocks // 2) for p in picks) + ((loads(every), shard_blocks),)


def count_of(mask, axis):
    return jnp.sum(mask.astype(jnp.int32), axis=axis, keepdims=True)


def total_of(mask, values, axis):
    return jnp.sum(jnp.where(mask, values, 0), axis=axis, keepdims=True)


def request_plan(blocks, seq, requests, length_ref, table_ref):
    me = lax.axis_index("seq")
    low = me * blocks
    square = (requests, requests)
    down = lax.broadcasted_iota(jnp.int32, square, 0)
    across = lax.broadcasted_iota(jnp.int32, square, 1)
    lane = lax.broadcasted_iota(jnp.int32, (1, requests), 1)
    lengths = jnp.broadcast_to(length_ref[...], square)
    length = total_of(down == across, lengths, 1)
    counts = (lengths + BLOCK - 1) // BLOCK
    ends = total_of(across <= down, counts, 1)
    starts = total_of(across < down, counts, 1)
    ends_row = total_of(down == across, jnp.broadcast_to(ends, square), 0)
    shard, shard_row = (ends - 1) // blocks, (ends_row - 1) // blocks
    place = count_of((down < across) & (shard == shard_row), 0)
    behind = me - shard_row
    behind = jnp.where(behind < 0, behind + seq, behind)
    half = seq // 2
    came_at = jnp.where(behind <= half, behind, half + seq - behind)
    block = low + lane
    member = (block >= starts) & (block < ends)
    request = jnp.minimum(count_of(ends <= block, 0), requests - 1)
    valid = total_of(member, jnp.clip(length - (block - starts) * BLOCK, 0, BLOCK), 0)
    begins = count_of(block == starts, 0)
    done = jnp.minimum(count_of(shard < me, 0) + lane, requests - 1)
    done_block = jnp.clip(total_of(down == done, ends, 0) - 1 - low, 0, blocks - 1)
    done_start = total_of(down == done, starts, 0)
    enters = [(done_start < low - back * blocks).astype(jnp.int32) for back in range(2)]
    for row, values in enumerate([came_at, place, request, valid, begins, done, done_block] + enters):
        table_ref[row : row + 1, 0:requests] = values
    return jnp.max(place, axis=1, keepdims=True) + 1


def ring_plan(schedules, seq, most_done, owner_ref, order_ref, plan_ref, found_ref):
    blocks = owner_ref.shape[0]
    capacity = order_ref.shape[1]
    shape = (blocks, seq)
    me = lax.axis_index("seq")
    down = lax.broadcasted_iota(jnp.int32, shape, 0)
    across = lax.broadcasted_iota(jnp.int32, shape, 1)
    owner = owner_ref[...]
    ahead = owner - across
    ahead = jnp.where(ahead < 0, ahead + seq, ahead)
    key = ahead * blocks + down
    order = jnp.zeros(shape, jnp.int32)
    for b in range(blocks):
        order = order + (key[b : b + 1] < key).astype(jnp.int32)
    moved = ahead > 0

    fitted = [None] * len(schedules)
    for split in SPLITS:
        right = ahead <= split
        rightward = count_of(right, 0)
        slot = jnp.where(right, rightward - 1 - order, order - rightward)
        steps = jnp.where(moved, jnp.where(right, ahead, seq - ahead), 0)
        for number, (used, _) in enumerate(schedules):
            excess = jnp.max(steps - travel(used, slot), axis=0, keepdims=True)
            fit = jnp.broadcast_to((excess <= 0).astype(jnp.int32), shape)
            now = (fit, slot, steps, right.astype(jnp.int32))
            if fitted[number] is None:
                fitted[number] = now
            else:
                before = fitted[number][0] > 0
                fitted[number] = tuple(jnp.where(before, f, n) for f, n in zip(fitted[number], now))

    mine = owner == me
    hot = mine.astype(jnp.float32)
    earlier = jnp.zeros(shape, jnp.float32)
    for b in range(blocks - 1):
        earlier = earlier + jnp.where(down > b, hot[b : b + 1], 0.0)
    each = jnp.broadcast_to(jnp.sum(hot, axis=0, keepdims=True), shape)
    ahead_of = lax.broadcasted_iota(jnp.int32, (seq, seq), 0) < lax.broadcasted_iota(jnp.int32, (seq, seq), 1)
    prior = jnp.dot(
        each.astype(jnp.bfloat16),
        ahead_of.astype(jnp.float32).astype(jnp.bfloat16),
        preferred_element_type=jnp.float32,
    )
    rank = (earlier + prior).astype(jnp.int32)
    row = jnp.full(shape, -1, jnp.int32)
    for k in range(capacity):
        row = jnp.where(mine & (rank == k), order_ref[me, k], row)

    tier = jnp.zeros((1, 1), jnp.int32)
    for number, (used, slots) in enumerate(schedules):
        fit, slot, steps, right = fitted[number]
        fits = jnp.min(fit[0:1], axis=1, keepdims=True) * (most_done <= slots).astype(jnp.int32)
        if number < len(schedules) - 1:
            tier = tier + 1 - fits
        wide, total = used[0], sum(used)
        begun = sum(jnp.where(steps > k + 1, n, 0) for k, n in enumerate(used))
        at = blocks + 1 + 2 * wide + jnp.where(right > 0, 0, total) + begun + slot
        at = jnp.where(moved, at, down)
        for c in range(capacity):
            found_ref[c : c + 1] = total_of(row == c, at + 1, 0)
        found = jnp.sum(found_ref[...], axis=1, keepdims=True)
        square = (capacity, capacity)
        diagonal = lax.broadcasted_iota(jnp.int32, square, 0) == lax.broadcasted_iota(jnp.int32, square, 1)
        source = total_of(diagonal, jnp.broadcast_to(found, square), 0)
        spot = jnp.where(moved, jnp.where(right > 0, 0, wide) + slot, -1)
        spot = total_of(across == me, spot + 1, 1) - 1
        plan_ref[2 * number : 2 * number + 1, 0:seq] = total_of(spot == across, down, 0)
        plan_ref[2 * number + 1 : 2 * number + 2, 0:capacity] = jnp.where(source > 0, source - 1, blocks)
    return tier


def exchange_kernel(
    tp, sub, groups, seq, requests, schedules,
    x_ref, owner_ref, length_ref, order_ref, query_ref, own_ref, tier_ref, plan_ref, table_ref, heads_ref,
    found, tiers, sem, send_sem, recv_sem, tier_send, tier_recv,
):
    group = lax.axis_index("groups")
    parts = head_parts(tp, sub, 0, x_ref, own_ref, sem, send_sem, recv_sem)
    others = [{"groups": lax.rem(group + step, groups)} for step in range(1, groups)]
    barrier = pltpu.get_barrier_semaphore()
    for where in head_peers(tp, sub) + others:
        pl.semaphore_signal(barrier, inc=1, device_id=where, device_id_type=MESH)
    pl.semaphore_wait(barrier, tp * sub + groups - 2)
    for part in parts:
        part.start()
    for head in range(heads_ref.shape[1]):
        heads_ref[:, head] = query_ref[:, head * HD : (head + 1) * HD].astype(jnp.float32)
    blocks = x_ref.shape[0]
    most_done = request_plan(blocks, seq, requests, length_ref, table_ref)
    tier = ring_plan(schedules, seq, most_done, owner_ref, order_ref, plan_ref, found)
    tiers[0] = jnp.broadcast_to(tier, tiers.shape[1:])
    told = [
        pltpu.make_async_remote_copy(
            src_ref=tiers.at[0],
            dst_ref=tiers.at[step + 1],
            send_sem=tier_send.at[step],
            recv_sem=tier_recv.at[step],
            device_id=where,
            device_id_type=MESH,
        )
        for step, where in enumerate(others)
    ]
    for part in told:
        part.start()
    for part in told + parts:
        part.wait()
    agreed = tiers[0]
    for step in range(len(others)):
        agreed = jnp.maximum(agreed, tiers[step + 1])
    tier_ref[0] = jnp.max(agreed)


def head_peers(tp, sub):
    me = lax.axis_index("tp") * sub + lax.axis_index("sub")
    others = [lax.rem(me + step, tp * sub) for step in range(1, tp * sub)]
    return [{"tp": other // sub, "sub": lax.rem(other, sub)} for other in others]


def head_parts(tp, sub, half, x_ref, own_ref, sem, send_sem, recv_sem):
    width = own_ref.shape[2]
    rows = x_ref.shape[2]
    me = lax.axis_index("tp") * sub + lax.axis_index("sub")
    mine = pl.ds(pl.multiple_of(me * rows, rows), rows)
    target = own_ref.at[:, mine, :]
    parts = [
        pltpu.make_async_copy(
            x_ref.at[:, half, :, pl.ds(pl.multiple_of(me * width, width), width)], target, sem
        )
    ]
    for step, where in enumerate(head_peers(tp, sub)):
        other = where["tp"] * sub + where["sub"]
        parts.append(
            pltpu.make_async_remote_copy(
                src_ref=x_ref.at[:, half, :, pl.ds(pl.multiple_of(other * width, width), width)],
                dst_ref=target,
                send_sem=send_sem.at[step],
                recv_sem=recv_sem.at[step],
                device_id=where,
                device_id_type=MESH,
            )
        )
    return parts


def exchange(prefill_kv, owners, lengths, slot_order, queries, schedules, tp, sub, groups, seq):
    blocks, _, rows, columns = prefill_kv.shape
    capacity = slot_order.shape[1]
    count = tp * sub
    requests = queries.shape[0]
    vmem = pl.BlockSpec(memory_space=pltpu.VMEM)
    return pl.pallas_call(
        functools.partial(exchange_kernel, tp, sub, groups, seq, requests, schedules),
        out_shape=(
            jax.ShapeDtypeStruct((blocks, rows * count, columns // count), prefill_kv.dtype),
            jax.ShapeDtypeStruct((1,), jnp.int32),
            jax.ShapeDtypeStruct((8, LANES), jnp.int32),
            jax.ShapeDtypeStruct((16, LANES), jnp.int32),
            jax.ShapeDtypeStruct((requests, queries.shape[1] // HD, HD), jnp.float32),
        ),
        in_specs=[pl.BlockSpec(memory_space=pl.ANY), vmem, vmem, pl.BlockSpec(memory_space=pltpu.SMEM), vmem],
        out_specs=[vmem, pl.BlockSpec(memory_space=pltpu.SMEM), vmem, vmem, vmem],
        scratch_shapes=[
            pltpu.VMEM((capacity, seq), jnp.int32),
            pltpu.VMEM((groups, 8, LANES), jnp.int32),
            pltpu.SemaphoreType.DMA,
            pltpu.SemaphoreType.DMA((count,)),
            pltpu.SemaphoreType.DMA((count,)),
            pltpu.SemaphoreType.DMA((groups,)),
            pltpu.SemaphoreType.DMA((groups,)),
        ],
        compiler_params=pltpu.CompilerParams(collective_id=0, has_side_effects=True),
    )(prefill_kv, owners, lengths, slot_order, queries)


def ring_kernel(
    used, slots, number, tp, sub, seq,
    x_ref, keys_ref, query_ref, new_ref, plan_ref, table_ref, cache_ref, rows_ref,
    klog, vlog, values, gathered, alog, states, came, sem, head_send, head_recv, send_sem, recv_sem, asend_sem, arecv_sem,
    state_send, state_recv,
):
    me = lax.axis_index("seq")

    def along(step):
        return {"seq": lax.rem(me + step + seq, seq)}

    blocks = keys_ref.shape[0]
    capacity, requests = cache_ref.shape[0], rows_ref.shape[0]
    group_size = query_ref.shape[1]
    wide, total = used[0], sum(used)
    starts = [sum(used[:k]) for k in range(len(used))]
    stage = blocks + 1
    base = (stage + 2 * wide, stage + 2 * wide + total)
    reach = (seq // 2, seq - 1 - seq // 2)
    logs = (klog, vlog)

    def stage_half(log, own_ref):
        log[blocks] = jnp.zeros(log.shape[1:], log.dtype)

        def keep(i, carry):
            log[i] = own_ref[i]
            return carry

        lax.fori_loop(0, blocks, keep, 0)

        def pick(i, carry):
            log[stage + i] = own_ref[plan_ref[2 * number, i]]
            return carry

        lax.fori_loop(0, 2 * wide, pick, 0)

    def block_copy(half, way, step, i):
        at = starts[step] + i
        source = stage + way * wide + i if step == 0 else base[way] + starts[step - 1] + i
        return pltpu.make_async_remote_copy(
            src_ref=logs[half].at[source],
            dst_ref=logs[half].at[base[way] + at],
            send_sem=send_sem.at[half, way],
            recv_sem=recv_sem.at[half, way, at],
            device_id=along((1, -1)[way]),
            device_id_type=MESH,
        )

    def forward(half, step):
        def body(i, carry):
            for way in range(2):
                if step > 0:
                    block_copy(half, way, step - 1, i).wait_recv()
                block_copy(half, way, step, i).start()
            return carry

        lax.fori_loop(0, used[step], body, 0)

    def land(half, step):
        beyond = used[step + 1] if step + 1 < len(used) else 0

        def body(i, carry):
            for way in range(2):
                block_copy(half, way, step, i).wait_recv()
            return carry

        lax.fori_loop(beyond, used[step], body, 0)

    def row_copy(way, step):
        at = way * reach[0] + step + 1
        source = 0 if step == 0 else at - 1
        return pltpu.make_async_remote_copy(
            src_ref=alog.at[pl.ds(source * slots, slots)],
            dst_ref=alog.at[pl.ds(at * slots, slots)],
            send_sem=asend_sem.at[at],
            recv_sem=arecv_sem.at[at],
            device_id=along((1, -1)[way]),
            device_id_type=MESH,
        )

    def state_copy(step):
        return pltpu.make_async_remote_copy(
            src_ref=states.at[blocks - 1],
            dst_ref=came.at[step],
            send_sem=state_send.at[step],
            recv_sem=state_recv.at[step],
            device_id=along(step + 1),
            device_id_type=MESH,
        )

    barrier = pltpu.get_barrier_semaphore()
    met = head_peers(tp, sub) + [along(step) for step in (1, -1, 2, -2)]
    for where in met:
        pl.semaphore_signal(barrier, inc=1, device_id=where, device_id_type=MESH)
    stage_half(klog, keys_ref)
    pl.semaphore_wait(barrier, len(met))

    parts = head_parts(tp, sub, 1, x_ref, values, sem, head_send, head_recv)
    for part in parts:
        part.start()
    forward(0, 0)

    scale = HD ** (-0.5)
    token = lax.broadcasted_iota(jnp.int32, (group_size, BLOCK), 1)
    weights, peaks, sums = [], [], []
    for b in range(blocks):
        query = query_ref[table_ref[2, b]].astype(jnp.bfloat16)
        score = scale * lax.dot_general(
            query, keys_ref[b], (((1,), (1,)), ((), ())), preferred_element_type=jnp.float32
        )
        score = jnp.where(token < table_ref[3, b], score, NEG_FLOOR)
        peak = jnp.max(score, axis=1, keepdims=True)
        weight = jnp.exp(score - peak).astype(jnp.bfloat16)
        weights.append(weight)
        peaks.append(jnp.broadcast_to(peak, (group_size, HD)))
        sums.append(
            jnp.broadcast_to(
                jnp.sum(weight.astype(jnp.float32), axis=1, keepdims=True), (group_size, HD)
            )
        )

    def merge(first, second):
        top = jnp.maximum(first[0], second[0])
        one, two = jnp.exp(first[0] - top), jnp.exp(second[0] - top)
        return (top, one * first[1] + two * second[1], one * first[2] + two * second[2])

    def attend():
        state = None
        for b in range(blocks):
            partial = jnp.dot(weights[b], values[b], preferred_element_type=jnp.float32)
            fresh = (peaks[b], sums[b], partial)
            if state is not None:
                begins = table_ref[4, b] > 0
                joined = merge(state, fresh)
                fresh = tuple(jnp.where(begins, f, j) for f, j in zip(fresh, joined))
            state = fresh
            for part in range(3):
                states[b, part] = state[part]

    def answer(j, carry):
        request = table_ref[5, j]
        block = table_ref[6, j]
        state = tuple(states[block, part] for part in range(3))
        for back in range(2):
            enters = table_ref[7 + back, j] > 0
            joined = merge(state, tuple(came[back, part] for part in range(3)))
            state = tuple(jnp.where(enters, f, s) for f, s in zip(joined, state))
        new = new_ref[request].astype(jnp.float32)
        own = scale * jnp.sum(
            query_ref[request] * new[0:1], axis=1, keepdims=True
        )
        own = jnp.broadcast_to(own, (group_size, HD))
        ones = jnp.ones((group_size, HD), jnp.float32)
        _, denom, numer = merge(state, (own, ones, jnp.broadcast_to(new[1:2], (group_size, HD))))
        alog[j] = (numer / denom).astype(alog.dtype)
        return carry

    lag = 3
    for turn in range(max(len(used) + 1, reach[0] + lag)):
        if 0 < turn < len(used):
            forward(0, turn)
        if turn == 1:
            for part in parts:
                part.wait()
            stage_half(vlog, values)
        if 0 < turn <= len(used):
            forward(1, turn - 1)
        if turn == 1:
            attend()
        if turn == 2:
            for step in range(2):
                state_copy(step).start()
        if turn == lag:
            for step in range(2):
                state_copy(step).wait()
            lax.fori_loop(0, slots, answer, 0)
        for way in range(2):
            if 0 <= turn - lag < reach[way]:
                if turn > lag:
                    row_copy(way, turn - lag - 1).wait_recv()
                row_copy(way, turn - lag).start()

    for half in range(2):
        for step in range(len(used)):
            land(half, step)

        def place(c, carry, half=half):
            cache_ref[c, half] = logs[half][plan_ref[2 * number + 1, c]]
            return carry

        lax.fori_loop(0, capacity, place, 0)
        if half == 0:
            for way in range(2):
                row_copy(way, reach[way] - 1).wait_recv()

            def collect(r, carry):
                gathered[r] = alog[table_ref[0, r] * slots + table_ref[1, r]].astype(jnp.float32)
                return carry

            lax.fori_loop(0, requests, collect, 0)
            for head in range(group_size):
                rows_ref[:, head * HD : (head + 1) * HD] = gathered[:, head].astype(rows_ref.dtype)
    for way in range(2):
        for step in range(reach[way]):
            row_copy(way, step).wait_send()
        for half in range(2):
            every = logs[half].at[pl.ds(base[way], total)]
            pltpu.make_async_remote_copy(
                src_ref=every,
                dst_ref=every,
                send_sem=send_sem.at[half, way],
                recv_sem=recv_sem.at[half, way, 0],
                device_id=along((1, -1)[way]),
                device_id_type=MESH,
            ).wait_send()

def ring(used, slots, number, tp, sub, seq, capacity, prefill_kv, keys, queries, new_kv, plan, table):
    blocks = keys.shape[0]
    wide, total = used[0], sum(used)
    requests, group_size = queries.shape[:2]
    count = tp * sub
    vmem = pl.BlockSpec(memory_space=pltpu.VMEM)
    smem = pl.BlockSpec(memory_space=pltpu.SMEM)
    log = pltpu.VMEM((blocks + 1 + 2 * wide + 2 * total,) + keys.shape[1:], keys.dtype)
    return pl.pallas_call(
        functools.partial(ring_kernel, used, slots, number, tp, sub, seq),
        out_shape=(
            jax.ShapeDtypeStruct((capacity, 2) + keys.shape[1:], keys.dtype),
            jax.ShapeDtypeStruct((requests, group_size * HD), jnp.bfloat16),
        ),
        in_specs=[pl.BlockSpec(memory_space=pl.ANY), vmem, vmem, vmem, smem, smem],
        out_specs=(vmem, vmem),
        scratch_shapes=[
            log,
            log,
            pltpu.VMEM(keys.shape, keys.dtype),
            pltpu.VMEM((requests, group_size, HD), jnp.float32),
            pltpu.VMEM((seq * slots, group_size, HD), jnp.bfloat16),
            pltpu.VMEM((blocks, 3, group_size, HD), jnp.float32),
            pltpu.VMEM((2, 3, group_size, HD), jnp.float32),
            pltpu.SemaphoreType.DMA,
            pltpu.SemaphoreType.DMA((count,)),
            pltpu.SemaphoreType.DMA((count,)),
            pltpu.SemaphoreType.DMA((2, 2)),
            pltpu.SemaphoreType.DMA((2, 2, total)),
            pltpu.SemaphoreType.DMA((seq,)),
            pltpu.SemaphoreType.DMA((seq,)),
            pltpu.SemaphoreType.DMA((2,)),
            pltpu.SemaphoreType.DMA((2,)),
        ],
        compiler_params=pltpu.CompilerParams(
            collective_id=number + 1, has_side_effects=True, vmem_limit_bytes=60 << 20
        ),
    )(prefill_kv, keys, queries, new_kv, plan, table)


def travel(used, slot):
    return sum((slot < n).astype(jnp.int32) for n in used)


def per_device(tp, sub, groups, seq, prefill_kv, prompt_lengths, block_owner, slot_order, queries, new_kv):
    shard_blocks = prefill_kv.shape[0]
    capacity = slot_order.shape[1]
    schedules = tiers(shard_blocks, seq)
    owners = block_owner.reshape(seq, shard_blocks).T
    keys, agreed, plan, table, query_rows = exchange(
        prefill_kv, owners, prompt_lengths[None], slot_order, queries, schedules, tp, sub, groups, seq
    )

    def deliver(number):
        used, slots = schedules[number]
        return ring(
            used, slots, number, tp, sub, seq, capacity,
            prefill_kv, keys, query_rows, new_kv, plan, table,
        )

    decode_cache, rows = lax.switch(
        agreed.reshape(()), [functools.partial(deliver, number) for number in range(len(schedules))]
    )
    return (decode_cache, rows)


def solution(mesh):
    return jax.shard_map(
        functools.partial(
            per_device, mesh.shape["tp"], mesh.shape["sub"], mesh.shape["groups"], mesh.shape["seq"]
        ),
        mesh=mesh,
        in_specs=(
            P(("groups", "seq"), None, ("tp", "sub"), None),
            P("groups"),
            P("groups"),
            P("groups", None),
            P("groups", ("tp", "sub")),
            P("groups", None, ("tp", "sub")),
        ),
        out_specs=(P(("groups", "seq"), None, None, ("tp", "sub")), P("groups", ("tp", "sub"))),
        check_vma=False,
    )
```

```python
import functools

import jax
import jax.numpy as jnp
from jax import lax
from jax.experimental import pallas as pl
from jax.experimental.pallas import tpu as pltpu
from jax.sharding import PartitionSpec as P

HD = 128
BLOCK = 128
NEG_FLOOR = -1e30
MESH = pl.DeviceIdType.MESH
SPLITS = (16, 15, 17, 14, 18, 13, 19, 12)
LANES = 128


def loads(steps_of_slot):
    return tuple(sum(c >= k for c in steps_of_slot) for k in range(1, max(steps_of_slot) + 1))


def tiers(shard_blocks, seq):
    half = seq // 2
    before = (7,) * (seq // 4)
    after = [
        [11, 9, 7, 6, 5, 4, 3, 2, 2, 1],
        [11, 9, 8, 7, 6, 5, 5, 4, 3, 2, 1],
    ]
    every = [half - i // 2 for i in range(shard_blocks)]
    return tuple((before, loads(p), shard_blocks // 2) for p in after) + ((loads(every), (), shard_blocks),)


def count_of(mask, axis):
    return jnp.sum(mask.astype(jnp.int32), axis=axis, keepdims=True)


def total_of(mask, values, axis):
    return jnp.sum(jnp.where(mask, values, 0), axis=axis, keepdims=True)


def request_plan(blocks, seq, requests, length_ref, table_ref):
    me = lax.axis_index("seq")
    low = me * blocks
    square = (requests, requests)
    down = lax.broadcasted_iota(jnp.int32, square, 0)
    across = lax.broadcasted_iota(jnp.int32, square, 1)
    lane = lax.broadcasted_iota(jnp.int32, (1, requests), 1)
    lengths = jnp.broadcast_to(length_ref[...], square)
    length = total_of(down == across, lengths, 1)
    counts = (lengths + BLOCK - 1) // BLOCK
    ends = total_of(across <= down, counts, 1)
    starts = total_of(across < down, counts, 1)
    ends_row = total_of(down == across, jnp.broadcast_to(ends, square), 0)
    shard, shard_row = (ends - 1) // blocks, (ends_row - 1) // blocks
    place = count_of((down < across) & (shard == shard_row), 0)
    behind = me - shard_row
    behind = jnp.where(behind < 0, behind + seq, behind)
    half = seq // 2
    came_at = jnp.where(behind <= half, behind, half + seq - behind)
    block = low + lane
    member = (block >= starts) & (block < ends)
    request = jnp.minimum(count_of(ends <= block, 0), requests - 1)
    valid = total_of(member, jnp.clip(length - (block - starts) * BLOCK, 0, BLOCK), 0)
    begins = count_of(block == starts, 0)
    done = jnp.minimum(count_of(shard < me, 0) + lane, requests - 1)
    done_block = jnp.clip(total_of(down == done, ends, 0) - 1 - low, 0, blocks - 1)
    done_start = total_of(down == done, starts, 0)
    enters = [(done_start < low - back * blocks).astype(jnp.int32) for back in range(2)]
    for row, values in enumerate([came_at, place, request, valid, begins, done, done_block] + enters):
        table_ref[row : row + 1, 0:requests] = values
    return jnp.max(place, axis=1, keepdims=True) + 1


def begun(used, steps):
    return sum(jnp.where(steps > k + 1, n, 0) for k, n in enumerate(used))


def whole_dot(values, matrix):
    product = jnp.dot(
        values.astype(jnp.float32).astype(jnp.bfloat16),
        matrix.astype(jnp.float32).astype(jnp.bfloat16),
        preferred_element_type=jnp.float32,
    )
    return product.astype(jnp.int32)


def ring_plan(schedules, seq, most_done, owner_ref, order_ref, plan_ref, found_ref):
    blocks = owner_ref.shape[0]
    capacity = order_ref.shape[1]
    shape = (blocks, seq)
    me = lax.axis_index("seq")
    down = lax.broadcasted_iota(jnp.int32, shape, 0)
    across = lax.broadcasted_iota(jnp.int32, shape, 1)
    from_lane = lax.broadcasted_iota(jnp.int32, (seq, seq), 0)
    to_lane = lax.broadcasted_iota(jnp.int32, (seq, seq), 1)
    owner = owner_ref[...]
    ahead = owner - across
    ahead = jnp.where(ahead < 0, ahead + seq, ahead)
    key = ahead * blocks + down
    order = jnp.zeros(shape, jnp.int32)
    for b in range(blocks):
        order = order + (key[b : b + 1] < key).astype(jnp.int32)
    moved = ahead > 0

    def routed(split):
        right = ahead <= split
        rightward = count_of(right, 0)
        slot = jnp.where(right, rightward - 1 - order, order - rightward)
        steps = jnp.where(moved, jnp.where(right, ahead, seq - ahead), 0)
        return slot, steps, right.astype(jnp.int32)

    best, cost = None, None
    for split in SPLITS:
        now = routed(split)
        share = (now[0] + 1).astype(jnp.float32) / (21 - now[1]).astype(jnp.float32)
        spent = jnp.max(jnp.where(moved, share, 0.0), axis=0, keepdims=True) + 0.002 * jnp.sum(
            now[1].astype(jnp.float32), axis=0, keepdims=True
        )
        spent = jnp.broadcast_to(spent, shape)
        if best is None:
            best, cost = now, spent
        else:
            less = spent < cost
            best = tuple(jnp.where(less, n, f) for n, f in zip(now, best))
            cost = jnp.where(less, spent, cost)

    mine = owner == me
    hot = mine.astype(jnp.float32)
    earlier = jnp.zeros(shape, jnp.float32)
    for b in range(blocks - 1):
        earlier = earlier + jnp.where(down > b, hot[b : b + 1], 0.0)
    each = jnp.broadcast_to(jnp.sum(hot, axis=0, keepdims=True), shape)
    rank = earlier.astype(jnp.int32) + whole_dot(each, from_lane < to_lane)
    row = jnp.full(shape, -1, jnp.int32)
    for k in range(capacity):
        row = jnp.where(mine & (rank == k), order_ref[me, k], row)

    def here(spot):
        return total_of(across == me, spot + 1, 1) - 1

    tier = jnp.zeros((1, 1), jnp.int32)
    for number, (first, second, slots) in enumerate(schedules):
        slot, steps, right = best if second else routed(seq // 2)
        wide, total = first[0], sum(first) + sum(second)
        wide_two = second[0] if second else 0
        turn = len(first)
        base = blocks + 1 + 2 * wide + 2 * wide_two
        at = base + jnp.where(right > 0, 0, total) + begun(first, steps) + slot
        sent = moved
        picks = jnp.zeros((1, seq), jnp.int32)
        fits = (most_done <= slots).astype(jnp.int32)
        if second:
            sent = moved & (slot < wide)
            for way in range(2):
                chosen = moved & (right == 1 - way)
                shift = to_lane - from_lane if way == 0 else from_lane - to_lane
                shifted = jnp.where(shift < 0, shift + seq, shift) == turn
                unshift = from_lane - to_lane if way == 0 else to_lane - from_lane
                unshifted = jnp.where(unshift < 0, unshift + seq, unshift) == turn
                on = chosen & sent & (steps > turn)
                left_on = whole_dot(jnp.where(on, steps - turn, 0), shifted)
                slot_on = whole_dot(jnp.where(on, slot, 0), shifted)
                left_late = jnp.where(chosen & (slot >= wide), steps, 0)
                key_on = left_on * (2 * blocks) + down
                key_late = left_late * (2 * blocks) + down + blocks
                rank_on = jnp.zeros(shape, jnp.int32)
                rank_late = jnp.zeros(shape, jnp.int32)
                for keys in (key_on, key_late):
                    for b in range(blocks):
                        rank_on = rank_on + (keys[b : b + 1] > key_on).astype(jnp.int32)
                        rank_late = rank_late + (keys[b : b + 1] > key_late).astype(jnp.int32)
                for left, place in ((left_on, rank_on), (left_late, rank_late)):
                    excess = jnp.where(left > 0, left - travel(second, place), 0)
                    excess = jnp.max(jnp.max(excess, axis=0, keepdims=True), axis=1, keepdims=True)
                    fits = fits * (excess <= 0).astype(jnp.int32)
                start = base + way * total + sum(first)
                rank_back = whole_dot(jnp.where(left_on > 0, rank_on, 0), unshifted)
                at = jnp.where(on, start + begun(second, steps - turn) + rank_back, at)
                at = jnp.where(left_late > 0, start + begun(second, left_late) + rank_late, at)
                for left, place, source in (
                    (left_on, rank_on, blocks + way * wide + slot_on),
                    (left_late, rank_late, down),
                ):
                    spot = here(jnp.where(left > 0, way * wide_two + place, -1))
                    value = here(source)
                    picks = picks + total_of(spot == across, jnp.broadcast_to(value, shape), 0)
        if number < len(schedules) - 1:
            tier = tier + 1 - fits
        at = jnp.where(moved, at, down)
        for c in range(capacity):
            found_ref[c : c + 1] = total_of(row == c, at + 1, 0)
        found = jnp.sum(found_ref[...], axis=1, keepdims=True)
        square = (capacity, capacity)
        diagonal = lax.broadcasted_iota(jnp.int32, square, 0) == lax.broadcasted_iota(jnp.int32, square, 1)
        source = total_of(diagonal, jnp.broadcast_to(found, square), 0)
        spot = here(jnp.where(sent, jnp.where(right > 0, 0, wide) + slot, -1))
        line = 3 * number
        plan_ref[line : line + 1, 0:seq] = total_of(spot == across, down, 0)
        plan_ref[line + 1 : line + 2, 0:capacity] = jnp.where(source > 0, source - 1, blocks)
        plan_ref[line + 2 : line + 3, 0:seq] = picks
    return tier


def exchange_kernel(
    tp, sub, groups, seq, requests, schedules,
    x_ref, owner_ref, length_ref, order_ref, query_ref, own_ref, tier_ref, plan_ref, table_ref, heads_ref,
    found, tiers, sem, send_sem, recv_sem, tier_send, tier_recv,
):
    group = lax.axis_index("groups")
    parts = head_parts(tp, sub, 0, x_ref, own_ref, sem, send_sem, recv_sem)
    others = [{"groups": lax.rem(group + step, groups)} for step in range(1, groups)]
    barrier = pltpu.get_barrier_semaphore()
    for where in head_peers(tp, sub) + others:
        pl.semaphore_signal(barrier, inc=1, device_id=where, device_id_type=MESH)
    pl.semaphore_wait(barrier, tp * sub + groups - 2)
    for part in parts:
        part.start()
    for head in range(heads_ref.shape[1]):
        heads_ref[:, head] = query_ref[:, head * HD : (head + 1) * HD].astype(jnp.float32)
    blocks = x_ref.shape[0]
    most_done = request_plan(blocks, seq, requests, length_ref, table_ref)
    tier = ring_plan(schedules, seq, most_done, owner_ref, order_ref, plan_ref, found)
    tiers[0] = jnp.broadcast_to(tier, tiers.shape[1:])
    told = [
        pltpu.make_async_remote_copy(
            src_ref=tiers.at[0],
            dst_ref=tiers.at[step + 1],
            send_sem=tier_send.at[step],
            recv_sem=tier_recv.at[step],
            device_id=where,
            device_id_type=MESH,
        )
        for step, where in enumerate(others)
    ]
    for part in told:
        part.start()
    for part in told + parts:
        part.wait()
    agreed = tiers[0]
    for step in range(len(others)):
        agreed = jnp.maximum(agreed, tiers[step + 1])
    tier_ref[0] = jnp.max(agreed)


def head_peers(tp, sub):
    me = lax.axis_index("tp") * sub + lax.axis_index("sub")
    others = [lax.rem(me + step, tp * sub) for step in range(1, tp * sub)]
    return [{"tp": other // sub, "sub": lax.rem(other, sub)} for other in others]


def head_parts(tp, sub, half, x_ref, own_ref, sem, send_sem, recv_sem):
    width = own_ref.shape[2]
    rows = x_ref.shape[2]
    me = lax.axis_index("tp") * sub + lax.axis_index("sub")
    mine = pl.ds(pl.multiple_of(me * rows, rows), rows)
    target = own_ref.at[:, mine, :]
    parts = [
        pltpu.make_async_copy(
            x_ref.at[:, half, :, pl.ds(pl.multiple_of(me * width, width), width)], target, sem
        )
    ]
    for step, where in enumerate(head_peers(tp, sub)):
        other = where["tp"] * sub + where["sub"]
        parts.append(
            pltpu.make_async_remote_copy(
                src_ref=x_ref.at[:, half, :, pl.ds(pl.multiple_of(other * width, width), width)],
                dst_ref=target,
                send_sem=send_sem.at[step],
                recv_sem=recv_sem.at[step],
                device_id=where,
                device_id_type=MESH,
            )
        )
    return parts


def exchange(prefill_kv, owners, lengths, slot_order, queries, schedules, tp, sub, groups, seq):
    blocks, _, rows, columns = prefill_kv.shape
    capacity = slot_order.shape[1]
    count = tp * sub
    requests = queries.shape[0]
    vmem = pl.BlockSpec(memory_space=pltpu.VMEM)
    return pl.pallas_call(
        functools.partial(exchange_kernel, tp, sub, groups, seq, requests, schedules),
        out_shape=(
            jax.ShapeDtypeStruct((blocks, rows * count, columns // count), prefill_kv.dtype),
            jax.ShapeDtypeStruct((1,), jnp.int32),
            jax.ShapeDtypeStruct((16, LANES), jnp.int32),
            jax.ShapeDtypeStruct((16, LANES), jnp.int32),
            jax.ShapeDtypeStruct((requests, queries.shape[1] // HD, HD), jnp.float32),
        ),
        in_specs=[pl.BlockSpec(memory_space=pl.ANY), vmem, vmem, pl.BlockSpec(memory_space=pltpu.SMEM), vmem],
        out_specs=[vmem, pl.BlockSpec(memory_space=pltpu.SMEM), vmem, vmem, vmem],
        scratch_shapes=[
            pltpu.VMEM((capacity, seq), jnp.int32),
            pltpu.VMEM((groups, 8, LANES), jnp.int32),
            pltpu.SemaphoreType.DMA,
            pltpu.SemaphoreType.DMA((count,)),
            pltpu.SemaphoreType.DMA((count,)),
            pltpu.SemaphoreType.DMA((groups,)),
            pltpu.SemaphoreType.DMA((groups,)),
        ],
        compiler_params=pltpu.CompilerParams(collective_id=0, has_side_effects=True),
    )(prefill_kv, owners, lengths, slot_order, queries)


def ring_kernel(
    first, second, slots, number, tp, sub, seq,
    x_ref, keys_ref, query_ref, new_ref, plan_ref, table_ref, cache_ref, rows_ref,
    klog, vlog, pool, values, gathered, alog, states, came, sem, head_send, head_recv, send_sem, recv_sem, asend_sem, arecv_sem,
    state_send, state_recv,
):
    me = lax.axis_index("seq")

    def along(step):
        return {"seq": lax.rem(me + step + seq, seq)}

    blocks = keys_ref.shape[0]
    capacity, requests = cache_ref.shape[0], rows_ref.shape[0]
    group_size = query_ref.shape[1]
    used, repack = first + second, len(first)
    total = sum(used)
    starts = [sum(used[:k]) for k in range(len(used))]
    line = 3 * number
    wide = {0: first[0]}
    stage = {0: blocks + 1}
    free = blocks + 1 + 2 * first[0]
    if second:
        wide[repack], stage[repack] = second[0], free
        free = free + 2 * second[0]
    base = (free, free + total)
    reach = (seq // 2, seq - 1 - seq // 2)
    logs = (klog, vlog)

    def stage_half(half, own_ref):
        log = logs[half]
        log[blocks] = jnp.zeros(log.shape[1:], log.dtype)

        def keep(i, carry):
            log[i] = own_ref[i]
            if second:
                pool[half, i] = own_ref[i]
            return carry

        lax.fori_loop(0, blocks, keep, 0)

        def pick(i, carry):
            log[stage[0] + i] = own_ref[plan_ref[line, i]]
            return carry

        lax.fori_loop(0, 2 * wide[0], pick, 0)

    def repack_half(half):
        log, step = logs[half], repack - 1

        def gather(i, carry):
            for way in range(2):
                block_copy(half, way, step, i).wait_recv()
                pool[half, blocks + way * used[step] + i] = log[base[way] + starts[step] + i]
            return carry

        lax.fori_loop(0, used[step], gather, 0)

        def pick(i, carry):
            log[stage[repack] + i] = pool[half, plan_ref[line + 2, i]]
            return carry

        lax.fori_loop(0, 2 * wide[repack], pick, 0)

    def block_copy(half, way, step, i):
        at = starts[step] + i
        if step in stage:
            source = stage[step] + way * wide[step] + i
        else:
            source = base[way] + starts[step - 1] + i
        return pltpu.make_async_remote_copy(
            src_ref=logs[half].at[source],
            dst_ref=logs[half].at[base[way] + at],
            send_sem=send_sem.at[half, way],
            recv_sem=recv_sem.at[half, way, at],
            device_id=along((1, -1)[way]),
            device_id_type=MESH,
        )

    def forward(half, step):
        if step > 0 and step in stage:
            repack_half(half)

        def body(i, carry):
            for way in range(2):
                if step not in stage:
                    block_copy(half, way, step - 1, i).wait_recv()
                block_copy(half, way, step, i).start()
            return carry

        lax.fori_loop(0, used[step], body, 0)

    def land(half, step):
        beyond = used[step + 1] if step + 1 < len(used) else 0
        if step + 1 in stage:
            beyond = used[step]

        def body(i, carry):
            for way in range(2):
                block_copy(half, way, step, i).wait_recv()
            return carry

        lax.fori_loop(beyond, used[step], body, 0)

    def row_copy(way, step):
        at = way * reach[0] + step + 1
        source = 0 if step == 0 else at - 1
        return pltpu.make_async_remote_copy(
            src_ref=alog.at[pl.ds(source * slots, slots)],
            dst_ref=alog.at[pl.ds(at * slots, slots)],
            send_sem=asend_sem.at[at],
            recv_sem=arecv_sem.at[at],
            device_id=along((1, -1)[way]),
            device_id_type=MESH,
        )

    def state_copy(step):
        return pltpu.make_async_remote_copy(
            src_ref=states.at[blocks - 1],
            dst_ref=came.at[step],
            send_sem=state_send.at[step],
            recv_sem=state_recv.at[step],
            device_id=along(step + 1),
            device_id_type=MESH,
        )

    barrier = pltpu.get_barrier_semaphore()
    met = head_peers(tp, sub) + [along(step) for step in (1, -1, 2, -2)]
    for where in met:
        pl.semaphore_signal(barrier, inc=1, device_id=where, device_id_type=MESH)
    stage_half(0, keys_ref)
    pl.semaphore_wait(barrier, len(met))

    parts = head_parts(tp, sub, 1, x_ref, values, sem, head_send, head_recv)
    for part in parts:
        part.start()
    forward(0, 0)

    scale = HD ** (-0.5)
    token = lax.broadcasted_iota(jnp.int32, (group_size, BLOCK), 1)
    weights, peaks, sums = [], [], []
    for b in range(blocks):
        query = query_ref[table_ref[2, b]].astype(jnp.bfloat16)
        score = scale * lax.dot_general(
            query, keys_ref[b], (((1,), (1,)), ((), ())), preferred_element_type=jnp.float32
        )
        score = jnp.where(token < table_ref[3, b], score, NEG_FLOOR)
        peak = jnp.max(score, axis=1, keepdims=True)
        weight = jnp.exp(score - peak).astype(jnp.bfloat16)
        weights.append(weight)
        peaks.append(jnp.broadcast_to(peak, (group_size, HD)))
        sums.append(
            jnp.broadcast_to(
                jnp.sum(weight.astype(jnp.float32), axis=1, keepdims=True), (group_size, HD)
            )
        )

    def merge(first, second):
        top = jnp.maximum(first[0], second[0])
        one, two = jnp.exp(first[0] - top), jnp.exp(second[0] - top)
        return (top, one * first[1] + two * second[1], one * first[2] + two * second[2])

    def attend():
        state = None
        for b in range(blocks):
            partial = jnp.dot(weights[b], values[b], preferred_element_type=jnp.float32)
            fresh = (peaks[b], sums[b], partial)
            if state is not None:
                begins = table_ref[4, b] > 0
                joined = merge(state, fresh)
                fresh = tuple(jnp.where(begins, f, j) for f, j in zip(fresh, joined))
            state = fresh
            for part in range(3):
                states[b, part] = state[part]

    def answer(j, carry):
        request = table_ref[5, j]
        block = table_ref[6, j]
        state = tuple(states[block, part] for part in range(3))
        for back in range(2):
            enters = table_ref[7 + back, j] > 0
            joined = merge(state, tuple(came[back, part] for part in range(3)))
            state = tuple(jnp.where(enters, f, s) for f, s in zip(joined, state))
        new = new_ref[request].astype(jnp.float32)
        own = scale * jnp.sum(
            query_ref[request] * new[0:1], axis=1, keepdims=True
        )
        own = jnp.broadcast_to(own, (group_size, HD))
        ones = jnp.ones((group_size, HD), jnp.float32)
        _, denom, numer = merge(state, (own, ones, jnp.broadcast_to(new[1:2], (group_size, HD))))
        alog[j] = (numer / denom).astype(alog.dtype)
        return carry

    lag = 3
    for turn in range(max(len(used) + 1, reach[0] + lag)):
        if 0 < turn < len(used):
            forward(0, turn)
        if turn == 1:
            for part in parts:
                part.wait()
            stage_half(1, values)
        if 0 < turn <= len(used):
            forward(1, turn - 1)
        if turn == 1:
            attend()
        if turn == 2:
            for step in range(2):
                state_copy(step).start()
        if turn == lag:
            for step in range(2):
                state_copy(step).wait()
            lax.fori_loop(0, slots, answer, 0)
        for way in range(2):
            if 0 <= turn - lag < reach[way]:
                if turn > lag:
                    row_copy(way, turn - lag - 1).wait_recv()
                row_copy(way, turn - lag).start()

    for half in range(2):
        for step in range(len(used)):
            land(half, step)

        def place(c, carry, half=half):
            cache_ref[c, half] = logs[half][plan_ref[line + 1, c]]
            return carry

        lax.fori_loop(0, capacity, place, 0)
        if half == 0:
            for way in range(2):
                row_copy(way, reach[way] - 1).wait_recv()

            def collect(r, carry):
                gathered[r] = alog[table_ref[0, r] * slots + table_ref[1, r]].astype(jnp.float32)
                return carry

            lax.fori_loop(0, requests, collect, 0)
            for head in range(group_size):
                rows_ref[:, head * HD : (head + 1) * HD] = gathered[:, head].astype(rows_ref.dtype)
    for way in range(2):
        for step in range(reach[way]):
            row_copy(way, step).wait_send()
        for half in range(2):
            every = logs[half].at[pl.ds(base[way], total)]
            pltpu.make_async_remote_copy(
                src_ref=every,
                dst_ref=every,
                send_sem=send_sem.at[half, way],
                recv_sem=recv_sem.at[half, way, 0],
                device_id=along((1, -1)[way]),
                device_id_type=MESH,
            ).wait_send()

def ring(first, second, slots, number, tp, sub, seq, capacity, prefill_kv, keys, queries, new_kv, plan, table):
    blocks = keys.shape[0]
    staged, total = first[0] + sum(second[:1]), sum(first) + sum(second)
    requests, group_size = queries.shape[:2]
    count = tp * sub
    vmem = pl.BlockSpec(memory_space=pltpu.VMEM)
    smem = pl.BlockSpec(memory_space=pltpu.SMEM)
    log = pltpu.VMEM((blocks + 1 + 2 * staged + 2 * total,) + keys.shape[1:], keys.dtype)
    return pl.pallas_call(
        functools.partial(ring_kernel, first, second, slots, number, tp, sub, seq),
        out_shape=(
            jax.ShapeDtypeStruct((capacity, 2) + keys.shape[1:], keys.dtype),
            jax.ShapeDtypeStruct((requests, group_size * HD), jnp.bfloat16),
        ),
        in_specs=[pl.BlockSpec(memory_space=pl.ANY), vmem, vmem, vmem, smem, smem],
        out_specs=(vmem, vmem),
        scratch_shapes=[
            log,
            log,
            pltpu.VMEM((2, blocks + 2 * first[-1]) + keys.shape[1:], keys.dtype),
            pltpu.VMEM(keys.shape, keys.dtype),
            pltpu.VMEM((requests, group_size, HD), jnp.float32),
            pltpu.VMEM((seq * slots, group_size, HD), jnp.bfloat16),
            pltpu.VMEM((blocks, 3, group_size, HD), jnp.float32),
            pltpu.VMEM((2, 3, group_size, HD), jnp.float32),
            pltpu.SemaphoreType.DMA,
            pltpu.SemaphoreType.DMA((count,)),
            pltpu.SemaphoreType.DMA((count,)),
            pltpu.SemaphoreType.DMA((2, 2)),
            pltpu.SemaphoreType.DMA((2, 2, total)),
            pltpu.SemaphoreType.DMA((seq,)),
            pltpu.SemaphoreType.DMA((seq,)),
            pltpu.SemaphoreType.DMA((2,)),
            pltpu.SemaphoreType.DMA((2,)),
        ],
        compiler_params=pltpu.CompilerParams(
            collective_id=number + 1, has_side_effects=True, vmem_limit_bytes=60 << 20
        ),
    )(prefill_kv, keys, queries, new_kv, plan, table)


def travel(used, slot):
    return sum((slot < n).astype(jnp.int32) for n in used)


def per_device(tp, sub, groups, seq, prefill_kv, prompt_lengths, block_owner, slot_order, queries, new_kv):
    shard_blocks = prefill_kv.shape[0]
    capacity = slot_order.shape[1]
    schedules = tiers(shard_blocks, seq)
    owners = block_owner.reshape(seq, shard_blocks).T
    keys, agreed, plan, table, query_rows = exchange(
        prefill_kv, owners, prompt_lengths[None], slot_order, queries, schedules, tp, sub, groups, seq
    )

    def deliver(number):
        first, second, slots = schedules[number]
        return ring(
            first, second, slots, number, tp, sub, seq, capacity,
            prefill_kv, keys, query_rows, new_kv, plan, table,
        )

    decode_cache, rows = lax.switch(
        agreed.reshape(()), [functools.partial(deliver, number) for number in range(len(schedules))]
    )
    return (decode_cache, rows)


def solution(mesh):
    return jax.shard_map(
        functools.partial(
            per_device, mesh.shape["tp"], mesh.shape["sub"], mesh.shape["groups"], mesh.shape["seq"]
        ),
        mesh=mesh,
        in_specs=(
            P(("groups", "seq"), None, ("tp", "sub"), None),
            P("groups"),
            P("groups"),
            P("groups", None),
            P("groups", ("tp", "sub")),
            P("groups", None, ("tp", "sub")),
        ),
        out_specs=(P(("groups", "seq"), None, None, ("tp", "sub")), P("groups", ("tp", "sub"))),
        check_vma=False,
    )
```

```python
import functools

import jax
import jax.numpy as jnp
from jax import lax
from jax.experimental import pallas as pl
from jax.experimental.pallas import tpu as pltpu
from jax.sharding import PartitionSpec as P

HD = 128
BLOCK = 128
NEG_FLOOR = -1e30
MESH = pl.DeviceIdType.MESH
SPLITS = (16, 15, 17, 14, 18, 13, 19, 12)
LANES = 128


def loads(steps_of_slot):
    return tuple(sum(c >= k for c in steps_of_slot) for k in range(1, max(steps_of_slot) + 1))


def tiers(shard_blocks, seq):
    half = seq // 2
    before = (7,) * (seq // 4)
    after = [
        [11, 9, 7, 6, 5, 4, 3, 2, 2, 1],
        [11, 9, 8, 7, 6, 5, 5, 4, 3, 2, 1],
    ]
    every = [half - i // 2 for i in range(shard_blocks)]
    return tuple((before, loads(p), shard_blocks // 2) for p in after) + ((loads(every), (), shard_blocks),)


def count_of(mask, axis):
    return jnp.sum(mask.astype(jnp.int32), axis=axis, keepdims=True)


def total_of(mask, values, axis):
    return jnp.sum(jnp.where(mask, values, 0), axis=axis, keepdims=True)


def request_plan(blocks, seq, requests, length_ref, table_ref):
    me = lax.axis_index("seq")
    low = me * blocks
    square = (requests, requests)
    down = lax.broadcasted_iota(jnp.int32, square, 0)
    across = lax.broadcasted_iota(jnp.int32, square, 1)
    lane = lax.broadcasted_iota(jnp.int32, (1, requests), 1)
    lengths = jnp.broadcast_to(length_ref[...], square)
    length = total_of(down == across, lengths, 1)
    counts = (lengths + BLOCK - 1) // BLOCK
    ends = total_of(across <= down, counts, 1)
    starts = total_of(across < down, counts, 1)
    ends_row = total_of(down == across, jnp.broadcast_to(ends, square), 0)
    shard, shard_row = (ends - 1) // blocks, (ends_row - 1) // blocks
    place = count_of((down < across) & (shard == shard_row), 0)
    behind = me - shard_row
    behind = jnp.where(behind < 0, behind + seq, behind)
    half = seq // 2
    came_at = jnp.where(behind <= half, behind, half + seq - behind)
    block = low + lane
    member = (block >= starts) & (block < ends)
    request = jnp.minimum(count_of(ends <= block, 0), requests - 1)
    valid = total_of(member, jnp.clip(length - (block - starts) * BLOCK, 0, BLOCK), 0)
    begins = count_of(block == starts, 0)
    done = jnp.minimum(count_of(shard < me, 0) + lane, requests - 1)
    done_block = jnp.clip(total_of(down == done, ends, 0) - 1 - low, 0, blocks - 1)
    done_start = total_of(down == done, starts, 0)
    enters = [(done_start < low - back * blocks).astype(jnp.int32) for back in range(2)]
    for row, values in enumerate([came_at, place, request, valid, begins, done, done_block] + enters):
        table_ref[row : row + 1, 0:requests] = values
    return jnp.max(place, axis=1, keepdims=True) + 1


def begun(used, steps):
    return sum(jnp.where(steps > k + 1, n, 0) for k, n in enumerate(used))


def whole_dot(values, matrix):
    product = jnp.dot(
        values.astype(jnp.float32).astype(jnp.bfloat16),
        matrix.astype(jnp.float32).astype(jnp.bfloat16),
        preferred_element_type=jnp.float32,
    )
    return product.astype(jnp.int32)


def ring_plan(schedules, seq, most_done, owner_ref, order_ref, plan_ref, found_ref):
    blocks = owner_ref.shape[0]
    capacity = order_ref.shape[1]
    shape = (blocks, seq)
    me = lax.axis_index("seq")
    down = lax.broadcasted_iota(jnp.int32, shape, 0)
    across = lax.broadcasted_iota(jnp.int32, shape, 1)
    from_lane = lax.broadcasted_iota(jnp.int32, (seq, seq), 0)
    to_lane = lax.broadcasted_iota(jnp.int32, (seq, seq), 1)
    owner = owner_ref[...]
    ahead = owner - across
    ahead = jnp.where(ahead < 0, ahead + seq, ahead)
    key = ahead * blocks + down
    order = jnp.zeros(shape, jnp.int32)
    for b in range(blocks):
        order = order + (key[b : b + 1] < key).astype(jnp.int32)
    moved = ahead > 0

    def routed(split):
        right = ahead <= split
        rightward = count_of(right, 0)
        slot = jnp.where(right, rightward - 1 - order, order - rightward)
        steps = jnp.where(moved, jnp.where(right, ahead, seq - ahead), 0)
        return slot, steps, right.astype(jnp.int32)

    best, cost = None, None
    for split in SPLITS:
        now = routed(split)
        share = (now[0] + 1).astype(jnp.float32) / (21 - now[1]).astype(jnp.float32)
        spent = jnp.max(jnp.where(moved, share, 0.0), axis=0, keepdims=True) + 0.002 * jnp.sum(
            now[1].astype(jnp.float32), axis=0, keepdims=True
        )
        spent = jnp.broadcast_to(spent, shape)
        if best is None:
            best, cost = now, spent
        else:
            less = spent < cost
            best = tuple(jnp.where(less, n, f) for n, f in zip(now, best))
            cost = jnp.where(less, spent, cost)

    mine = owner == me
    hot = mine.astype(jnp.float32)
    earlier = jnp.zeros(shape, jnp.float32)
    for b in range(blocks - 1):
        earlier = earlier + jnp.where(down > b, hot[b : b + 1], 0.0)
    each = jnp.broadcast_to(jnp.sum(hot, axis=0, keepdims=True), shape)
    rank = earlier.astype(jnp.int32) + whole_dot(each, from_lane < to_lane)
    row = jnp.full(shape, -1, jnp.int32)
    for k in range(capacity):
        row = jnp.where(mine & (rank == k), order_ref[me, k], row)

    def here(spot):
        return total_of(across == me, spot + 1, 1) - 1

    tier = jnp.zeros((1, 1), jnp.int32)
    for number, (first, second, slots) in enumerate(schedules):
        slot, steps, right = best if second else routed(seq // 2)
        wide, total = first[0], sum(first) + sum(second)
        wide_two = second[0] if second else 0
        turn = len(first)
        base = blocks + 1 + 2 * wide + 2 * wide_two
        at = base + jnp.where(right > 0, 0, total) + begun(first, steps) + slot
        sent = moved
        picks = jnp.zeros((1, seq), jnp.int32)
        fits = (most_done <= slots).astype(jnp.int32)
        if second:
            sent = moved & (slot < wide)
            for way in range(2):
                chosen = moved & (right == 1 - way)
                shift = to_lane - from_lane if way == 0 else from_lane - to_lane
                shifted = jnp.where(shift < 0, shift + seq, shift) == turn
                unshift = from_lane - to_lane if way == 0 else to_lane - from_lane
                unshifted = jnp.where(unshift < 0, unshift + seq, unshift) == turn
                on = chosen & sent & (steps > turn)
                left_on = whole_dot(jnp.where(on, steps - turn, 0), shifted)
                slot_on = whole_dot(jnp.where(on, slot, 0), shifted)
                left_late = jnp.where(chosen & (slot >= wide), steps, 0)
                key_on = left_on * (2 * blocks) + down
                key_late = left_late * (2 * blocks) + down + blocks
                rank_on = jnp.zeros(shape, jnp.int32)
                rank_late = jnp.zeros(shape, jnp.int32)
                for keys in (key_on, key_late):
                    for b in range(blocks):
                        rank_on = rank_on + (keys[b : b + 1] > key_on).astype(jnp.int32)
                        rank_late = rank_late + (keys[b : b + 1] > key_late).astype(jnp.int32)
                for left, place in ((left_on, rank_on), (left_late, rank_late)):
                    excess = jnp.where(left > 0, left - travel(second, place), 0)
                    excess = jnp.max(jnp.max(excess, axis=0, keepdims=True), axis=1, keepdims=True)
                    fits = fits * (excess <= 0).astype(jnp.int32)
                start = base + way * total + sum(first)
                rank_back = whole_dot(jnp.where(left_on > 0, rank_on, 0), unshifted)
                at = jnp.where(on, start + begun(second, steps - turn) + rank_back, at)
                at = jnp.where(left_late > 0, start + begun(second, left_late) + rank_late, at)
                for left, place, source in (
                    (left_on, rank_on, blocks + way * wide + slot_on),
                    (left_late, rank_late, down),
                ):
                    spot = here(jnp.where(left > 0, way * wide_two + place, -1))
                    value = here(source)
                    picks = picks + total_of(spot == across, jnp.broadcast_to(value, shape), 0)
        if number < len(schedules) - 1:
            tier = tier + 1 - fits
        at = jnp.where(moved, at, down)
        for c in range(capacity):
            found_ref[c : c + 1] = total_of(row == c, at + 1, 0)
        found = jnp.sum(found_ref[...], axis=1, keepdims=True)
        square = (capacity, capacity)
        diagonal = lax.broadcasted_iota(jnp.int32, square, 0) == lax.broadcasted_iota(jnp.int32, square, 1)
        source = total_of(diagonal, jnp.broadcast_to(found, square), 0)
        spot = here(jnp.where(sent, jnp.where(right > 0, 0, wide) + slot, -1))
        line = 3 * number
        plan_ref[line : line + 1, 0:seq] = total_of(spot == across, down, 0)
        plan_ref[line + 1 : line + 2, 0:capacity] = jnp.where(source > 0, source - 1, blocks)
        plan_ref[line + 2 : line + 3, 0:seq] = picks
    return tier


def exchange_kernel(
    tp, sub, groups, seq, requests, schedules,
    x_ref, owner_ref, length_ref, order_ref, query_ref, own_ref, tier_ref, plan_ref, table_ref, heads_ref,
    found, tiers, sem, send_sem, recv_sem, tier_send, tier_recv,
):
    group = lax.axis_index("groups")
    parts = head_parts(tp, sub, 0, x_ref, own_ref, sem, send_sem, recv_sem)
    others = [{"groups": lax.rem(group + step, groups)} for step in range(1, groups)]
    barrier = pltpu.get_barrier_semaphore()
    for where in head_peers(tp, sub) + others:
        pl.semaphore_signal(barrier, inc=1, device_id=where, device_id_type=MESH)
    pl.semaphore_wait(barrier, tp * sub + groups - 2)
    for part in parts:
        part.start()
    for head in range(heads_ref.shape[1]):
        heads_ref[:, head] = query_ref[:, head * HD : (head + 1) * HD].astype(jnp.float32)
    blocks = x_ref.shape[0]
    most_done = request_plan(blocks, seq, requests, length_ref, table_ref)
    tier = ring_plan(schedules, seq, most_done, owner_ref, order_ref, plan_ref, found)
    tiers[0] = jnp.broadcast_to(tier, tiers.shape[1:])
    told = [
        pltpu.make_async_remote_copy(
            src_ref=tiers.at[0],
            dst_ref=tiers.at[step + 1],
            send_sem=tier_send.at[step],
            recv_sem=tier_recv.at[step],
            device_id=where,
            device_id_type=MESH,
        )
        for step, where in enumerate(others)
    ]
    for part in told:
        part.start()
    for part in told + parts:
        part.wait()
    agreed = tiers[0]
    for step in range(len(others)):
        agreed = jnp.maximum(agreed, tiers[step + 1])
    tier_ref[0] = jnp.max(agreed)


def head_peers(tp, sub):
    me = lax.axis_index("tp") * sub + lax.axis_index("sub")
    others = [lax.rem(me + step, tp * sub) for step in range(1, tp * sub)]
    return [{"tp": other // sub, "sub": lax.rem(other, sub)} for other in others]


def head_parts(tp, sub, half, x_ref, own_ref, sem, send_sem, recv_sem):
    width = own_ref.shape[2]
    rows = x_ref.shape[2]
    me = lax.axis_index("tp") * sub + lax.axis_index("sub")
    mine = pl.ds(pl.multiple_of(me * rows, rows), rows)
    target = own_ref.at[:, mine, :]
    parts = [
        pltpu.make_async_copy(
            x_ref.at[:, half, :, pl.ds(pl.multiple_of(me * width, width), width)], target, sem
        )
    ]
    for step, where in enumerate(head_peers(tp, sub)):
        other = where["tp"] * sub + where["sub"]
        parts.append(
            pltpu.make_async_remote_copy(
                src_ref=x_ref.at[:, half, :, pl.ds(pl.multiple_of(other * width, width), width)],
                dst_ref=target,
                send_sem=send_sem.at[step],
                recv_sem=recv_sem.at[step],
                device_id=where,
                device_id_type=MESH,
            )
        )
    return parts


def exchange(prefill_kv, owners, lengths, slot_order, queries, schedules, tp, sub, groups, seq):
    blocks, _, rows, columns = prefill_kv.shape
    capacity = slot_order.shape[1]
    count = tp * sub
    requests = queries.shape[0]
    vmem = pl.BlockSpec(memory_space=pltpu.VMEM)
    return pl.pallas_call(
        functools.partial(exchange_kernel, tp, sub, groups, seq, requests, schedules),
        out_shape=(
            jax.ShapeDtypeStruct((blocks, rows * count, columns // count), prefill_kv.dtype),
            jax.ShapeDtypeStruct((1,), jnp.int32),
            jax.ShapeDtypeStruct((16, LANES), jnp.int32),
            jax.ShapeDtypeStruct((16, LANES), jnp.int32),
            jax.ShapeDtypeStruct((requests, queries.shape[1] // HD, HD), jnp.float32),
        ),
        in_specs=[pl.BlockSpec(memory_space=pl.ANY), vmem, vmem, pl.BlockSpec(memory_space=pltpu.SMEM), vmem],
        out_specs=[vmem, pl.BlockSpec(memory_space=pltpu.SMEM), vmem, vmem, vmem],
        scratch_shapes=[
            pltpu.VMEM((capacity, seq), jnp.int32),
            pltpu.VMEM((groups, 8, LANES), jnp.int32),
            pltpu.SemaphoreType.DMA,
            pltpu.SemaphoreType.DMA((count,)),
            pltpu.SemaphoreType.DMA((count,)),
            pltpu.SemaphoreType.DMA((groups,)),
            pltpu.SemaphoreType.DMA((groups,)),
        ],
        compiler_params=pltpu.CompilerParams(collective_id=0, has_side_effects=True),
    )(prefill_kv, owners, lengths, slot_order, queries)


def ring_kernel(
    first, second, slots, number, tp, sub, seq,
    x_ref, keys_ref, query_ref, new_ref, plan_ref, table_ref, cache_ref, rows_ref,
    klog, vlog, pool, values, gathered, alog, states, came, sem, head_send, head_recv, send_sem, recv_sem, asend_sem, arecv_sem,
    state_send, state_recv,
):
    me = lax.axis_index("seq")

    def along(step):
        return {"seq": lax.rem(me + step + seq, seq)}

    blocks = keys_ref.shape[0]
    capacity, requests = cache_ref.shape[0], rows_ref.shape[0]
    group_size = query_ref.shape[1]
    used, repack = first + second, len(first)
    total = sum(used)
    starts = [sum(used[:k]) for k in range(len(used))]
    line = 3 * number
    wide = {0: first[0]}
    stage = {0: blocks + 1}
    free = blocks + 1 + 2 * first[0]
    if second:
        wide[repack], stage[repack] = second[0], free
        free = free + 2 * second[0]
    base = (free, free + total)
    reach = (seq // 2, seq - 1 - seq // 2)
    logs = (klog, vlog)

    def stage_half(half, own_ref):
        log = logs[half]
        log[blocks] = jnp.zeros(log.shape[1:], log.dtype)

        def keep(i, carry):
            log[i] = own_ref[i]
            if second:
                pool[half, i] = own_ref[i]
            return carry

        lax.fori_loop(0, blocks, keep, 0)

        def pick(i, carry):
            log[stage[0] + i] = own_ref[plan_ref[line, i]]
            return carry

        lax.fori_loop(0, 2 * wide[0], pick, 0)

    def repack_half(half):
        log, step = logs[half], repack - 1

        def gather(i, carry):
            for way in range(2):
                block_copy(half, way, step, i).wait_recv()
                pool[half, blocks + way * used[step] + i] = log[base[way] + starts[step] + i]
            return carry

        lax.fori_loop(0, used[step], gather, 0)

        def pick(i, carry):
            log[stage[repack] + i] = pool[half, plan_ref[line + 2, i]]
            return carry

        lax.fori_loop(0, 2 * wide[repack], pick, 0)

    def block_copy(half, way, step, i):
        at = starts[step] + i
        if step in stage:
            source = stage[step] + way * wide[step] + i
        else:
            source = base[way] + starts[step - 1] + i
        return pltpu.make_async_remote_copy(
            src_ref=logs[half].at[source],
            dst_ref=logs[half].at[base[way] + at],
            send_sem=send_sem.at[half, way],
            recv_sem=recv_sem.at[half, way, at],
            device_id=along((1, -1)[way]),
            device_id_type=MESH,
        )

    def hop(half, step, low, high):
        def body(i, carry):
            for way in range(2):
                if step not in stage:
                    block_copy(half, way, step - 1, i).wait_recv()
                block_copy(half, way, step, i).start()
            return carry

        if low < high:
            lax.fori_loop(low, high, body, 0)

    express, doubled = 2, 4
    turns = len(used)
    if second:
        turns = repack + max(sum(n > express for n in second), len(second) - doubled)

    def forward(half, turn):
        if turn > 0 and turn in stage:
            repack_half(half)
        if not second or turn < repack:
            hop(half, turn, 0, used[turn])
            return
        late = turn - repack
        step = repack + late + min(late, doubled)
        if step < len(used):
            hop(half, step, 0, min(express, used[step]))
        if turn < len(used):
            hop(half, turn, express, used[turn])
        if late < doubled and step + 1 < len(used):
            hop(half, step + 1, 0, min(express, used[step + 1]))

    def land(half, step):
        beyond = used[step + 1] if step + 1 < len(used) else 0
        if step + 1 in stage:
            beyond = used[step]

        def body(i, carry):
            for way in range(2):
                block_copy(half, way, step, i).wait_recv()
            return carry

        lax.fori_loop(beyond, used[step], body, 0)

    def row_copy(way, step):
        at = way * reach[0] + step + 1
        source = 0 if step == 0 else at - 1
        return pltpu.make_async_remote_copy(
            src_ref=alog.at[pl.ds(source * slots, slots)],
            dst_ref=alog.at[pl.ds(at * slots, slots)],
            send_sem=asend_sem.at[at],
            recv_sem=arecv_sem.at[at],
            device_id=along((1, -1)[way]),
            device_id_type=MESH,
        )

    def state_copy(step):
        return pltpu.make_async_remote_copy(
            src_ref=states.at[blocks - 1],
            dst_ref=came.at[step],
            send_sem=state_send.at[step],
            recv_sem=state_recv.at[step],
            device_id=along(step + 1),
            device_id_type=MESH,
        )

    barrier = pltpu.get_barrier_semaphore()
    met = head_peers(tp, sub) + [along(step) for step in (1, -1, 2, -2)]
    for where in met:
        pl.semaphore_signal(barrier, inc=1, device_id=where, device_id_type=MESH)
    stage_half(0, keys_ref)
    pl.semaphore_wait(barrier, len(met))

    parts = head_parts(tp, sub, 1, x_ref, values, sem, head_send, head_recv)
    for part in parts:
        part.start()
    forward(0, 0)

    scale = HD ** (-0.5)
    token = lax.broadcasted_iota(jnp.int32, (group_size, BLOCK), 1)
    weights, peaks, sums = [], [], []
    for b in range(blocks):
        query = query_ref[table_ref[2, b]].astype(jnp.bfloat16)
        score = scale * lax.dot_general(
            query, keys_ref[b], (((1,), (1,)), ((), ())), preferred_element_type=jnp.float32
        )
        score = jnp.where(token < table_ref[3, b], score, NEG_FLOOR)
        peak = jnp.max(score, axis=1, keepdims=True)
        weight = jnp.exp(score - peak).astype(jnp.bfloat16)
        weights.append(weight)
        peaks.append(jnp.broadcast_to(peak, (group_size, HD)))
        sums.append(
            jnp.broadcast_to(
                jnp.sum(weight.astype(jnp.float32), axis=1, keepdims=True), (group_size, HD)
            )
        )

    def merge(first, second):
        top = jnp.maximum(first[0], second[0])
        one, two = jnp.exp(first[0] - top), jnp.exp(second[0] - top)
        return (top, one * first[1] + two * second[1], one * first[2] + two * second[2])

    def attend():
        state = None
        for b in range(blocks):
            partial = jnp.dot(weights[b], values[b], preferred_element_type=jnp.float32)
            fresh = (peaks[b], sums[b], partial)
            if state is not None:
                begins = table_ref[4, b] > 0
                joined = merge(state, fresh)
                fresh = tuple(jnp.where(begins, f, j) for f, j in zip(fresh, joined))
            state = fresh
            for part in range(3):
                states[b, part] = state[part]

    def answer(j, carry):
        request = table_ref[5, j]
        block = table_ref[6, j]
        state = tuple(states[block, part] for part in range(3))
        for back in range(2):
            enters = table_ref[7 + back, j] > 0
            joined = merge(state, tuple(came[back, part] for part in range(3)))
            state = tuple(jnp.where(enters, f, s) for f, s in zip(joined, state))
        new = new_ref[request].astype(jnp.float32)
        own = scale * jnp.sum(
            query_ref[request] * new[0:1], axis=1, keepdims=True
        )
        own = jnp.broadcast_to(own, (group_size, HD))
        ones = jnp.ones((group_size, HD), jnp.float32)
        _, denom, numer = merge(state, (own, ones, jnp.broadcast_to(new[1:2], (group_size, HD))))
        alog[j] = (numer / denom).astype(alog.dtype)
        return carry

    def row_hop(step):
        for way in range(2):
            if step < reach[way]:
                if step > 0:
                    row_copy(way, step - 1).wait_recv()
                row_copy(way, step).start()

    lag, rows_sent = 3, 0
    for turn in range(turns + 1):
        if 0 < turn < turns:
            forward(0, turn)
        if second and repack <= turn < turns and rows_sent < reach[0]:
            row_hop(rows_sent)
            rows_sent += 1
        if turn == 1:
            for part in parts:
                part.wait()
            stage_half(1, values)
        if 0 < turn <= turns:
            forward(1, turn - 1)
        if turn == 1:
            attend()
        if turn == 2:
            for step in range(2):
                state_copy(step).start()
        if turn == lag:
            for step in range(2):
                state_copy(step).wait()
            lax.fori_loop(0, slots, answer, 0)
        if turn >= lag and rows_sent < reach[0]:
            row_hop(rows_sent)
            rows_sent += 1
    for step in range(rows_sent, reach[0]):
        row_hop(step)

    for half in range(2):
        for step in range(len(used)):
            land(half, step)

        def place(c, carry, half=half):
            cache_ref[c, half] = logs[half][plan_ref[line + 1, c]]
            return carry

        lax.fori_loop(0, capacity, place, 0)
        if half == 0:
            for way in range(2):
                row_copy(way, reach[way] - 1).wait_recv()

            def collect(r, carry):
                gathered[r] = alog[table_ref[0, r] * slots + table_ref[1, r]].astype(jnp.float32)
                return carry

            lax.fori_loop(0, requests, collect, 0)
            for head in range(group_size):
                rows_ref[:, head * HD : (head + 1) * HD] = gathered[:, head].astype(rows_ref.dtype)
    for way in range(2):
        for step in range(reach[way]):
            row_copy(way, step).wait_send()
        for half in range(2):
            every = logs[half].at[pl.ds(base[way], total)]
            pltpu.make_async_remote_copy(
                src_ref=every,
                dst_ref=every,
                send_sem=send_sem.at[half, way],
                recv_sem=recv_sem.at[half, way, 0],
                device_id=along((1, -1)[way]),
                device_id_type=MESH,
            ).wait_send()

def ring(first, second, slots, number, tp, sub, seq, capacity, prefill_kv, keys, queries, new_kv, plan, table):
    blocks = keys.shape[0]
    staged, total = first[0] + sum(second[:1]), sum(first) + sum(second)
    requests, group_size = queries.shape[:2]
    count = tp * sub
    vmem = pl.BlockSpec(memory_space=pltpu.VMEM)
    smem = pl.BlockSpec(memory_space=pltpu.SMEM)
    log = pltpu.VMEM((blocks + 1 + 2 * staged + 2 * total,) + keys.shape[1:], keys.dtype)
    return pl.pallas_call(
        functools.partial(ring_kernel, first, second, slots, number, tp, sub, seq),
        out_shape=(
            jax.ShapeDtypeStruct((capacity, 2) + keys.shape[1:], keys.dtype),
            jax.ShapeDtypeStruct((requests, group_size * HD), jnp.bfloat16),
        ),
        in_specs=[pl.BlockSpec(memory_space=pl.ANY), vmem, vmem, vmem, smem, smem],
        out_specs=(vmem, vmem),
        scratch_shapes=[
            log,
            log,
            pltpu.VMEM((2, blocks + 2 * first[-1]) + keys.shape[1:], keys.dtype),
            pltpu.VMEM(keys.shape, keys.dtype),
            pltpu.VMEM((requests, group_size, HD), jnp.float32),
            pltpu.VMEM((seq * slots, group_size, HD), jnp.bfloat16),
            pltpu.VMEM((blocks, 3, group_size, HD), jnp.float32),
            pltpu.VMEM((2, 3, group_size, HD), jnp.float32),
            pltpu.SemaphoreType.DMA,
            pltpu.SemaphoreType.DMA((count,)),
            pltpu.SemaphoreType.DMA((count,)),
            pltpu.SemaphoreType.DMA((2, 2)),
            pltpu.SemaphoreType.DMA((2, 2, total)),
            pltpu.SemaphoreType.DMA((seq,)),
            pltpu.SemaphoreType.DMA((seq,)),
            pltpu.SemaphoreType.DMA((2,)),
            pltpu.SemaphoreType.DMA((2,)),
        ],
        compiler_params=pltpu.CompilerParams(
            collective_id=number + 1, has_side_effects=True, vmem_limit_bytes=60 << 20
        ),
    )(prefill_kv, keys, queries, new_kv, plan, table)


def travel(used, slot):
    return sum((slot < n).astype(jnp.int32) for n in used)


def per_device(tp, sub, groups, seq, prefill_kv, prompt_lengths, block_owner, slot_order, queries, new_kv):
    shard_blocks = prefill_kv.shape[0]
    capacity = slot_order.shape[1]
    schedules = tiers(shard_blocks, seq)
    owners = block_owner.reshape(seq, shard_blocks).T
    keys, agreed, plan, table, query_rows = exchange(
        prefill_kv, owners, prompt_lengths[None], slot_order, queries, schedules, tp, sub, groups, seq
    )

    def deliver(number):
        first, second, slots = schedules[number]
        return ring(
            first, second, slots, number, tp, sub, seq, capacity,
            prefill_kv, keys, query_rows, new_kv, plan, table,
        )

    decode_cache, rows = lax.switch(
        agreed.reshape(()), [functools.partial(deliver, number) for number in range(len(schedules))]
    )
    return (decode_cache, rows)


def solution(mesh):
    return jax.shard_map(
        functools.partial(
            per_device, mesh.shape["tp"], mesh.shape["sub"], mesh.shape["groups"], mesh.shape["seq"]
        ),
        mesh=mesh,
        in_specs=(
            P(("groups", "seq"), None, ("tp", "sub"), None),
            P("groups"),
            P("groups"),
            P("groups", None),
            P("groups", ("tp", "sub")),
            P("groups", None, ("tp", "sub")),
        ),
        out_specs=(P(("groups", "seq"), None, None, ("tp", "sub")), P("groups", ("tp", "sub"))),
        check_vma=False,
    )
```

```python
import functools

import jax
import jax.numpy as jnp
from jax import lax
from jax.experimental import pallas as pl
from jax.experimental.pallas import tpu as pltpu
from jax.sharding import PartitionSpec as P

HD = 128
BLOCK = 128
NEG_FLOOR = -1e30
MESH = pl.DeviceIdType.MESH
SPLITS = (16, 15, 17, 14, 18, 13, 19, 12)
LANES = 128


def loads(steps_of_slot):
    return tuple(sum(c >= k for c in steps_of_slot) for k in range(1, max(steps_of_slot) + 1))


def tiers(shard_blocks, seq):
    half = seq // 2
    before = (7,) * (seq // 4)
    after = [
        [11, 9, 7, 6, 5, 4, 3, 2, 2, 1],
        [11, 9, 8, 7, 6, 5, 4, 3, 2, 1],
        [11, 9, 8, 7, 6, 5, 5, 4, 3, 2, 1],
    ]
    every = [half - i // 2 for i in range(shard_blocks)]
    return tuple((before, loads(p), shard_blocks // 2) for p in after) + ((loads(every), (), shard_blocks),)


def count_of(mask, axis):
    return jnp.sum(mask.astype(jnp.int32), axis=axis, keepdims=True)


def total_of(mask, values, axis):
    return jnp.sum(jnp.where(mask, values, 0), axis=axis, keepdims=True)


def request_plan(blocks, seq, requests, length_ref, table_ref):
    me = lax.axis_index("seq")
    low = me * blocks
    square = (requests, requests)
    down = lax.broadcasted_iota(jnp.int32, square, 0)
    across = lax.broadcasted_iota(jnp.int32, square, 1)
    lane = lax.broadcasted_iota(jnp.int32, (1, requests), 1)
    lengths = jnp.broadcast_to(length_ref[...], square)
    length = total_of(down == across, lengths, 1)
    counts = (lengths + BLOCK - 1) // BLOCK
    ends = total_of(across <= down, counts, 1)
    starts = total_of(across < down, counts, 1)
    ends_row = total_of(down == across, jnp.broadcast_to(ends, square), 0)
    shard, shard_row = (ends - 1) // blocks, (ends_row - 1) // blocks
    place = count_of((down < across) & (shard == shard_row), 0)
    behind = me - shard_row
    behind = jnp.where(behind < 0, behind + seq, behind)
    half = seq // 2
    came_at = jnp.where(behind <= half, behind, half + seq - behind)
    block = low + lane
    member = (block >= starts) & (block < ends)
    request = jnp.minimum(count_of(ends <= block, 0), requests - 1)
    valid = total_of(member, jnp.clip(length - (block - starts) * BLOCK, 0, BLOCK), 0)
    begins = count_of(block == starts, 0)
    done = jnp.minimum(count_of(shard < me, 0) + lane, requests - 1)
    done_block = jnp.clip(total_of(down == done, ends, 0) - 1 - low, 0, blocks - 1)
    done_start = total_of(down == done, starts, 0)
    enters = [(done_start < low - back * blocks).astype(jnp.int32) for back in range(2)]
    for row, values in enumerate([came_at, place, request, valid, begins, done, done_block] + enters):
        table_ref[row : row + 1, 0:requests] = values
    return jnp.max(place, axis=1, keepdims=True) + 1


def begun(used, steps):
    return sum(jnp.where(steps > k + 1, n, 0) for k, n in enumerate(used))


def whole_dot(values, matrix):
    product = jnp.dot(
        values.astype(jnp.float32).astype(jnp.bfloat16),
        matrix.astype(jnp.float32).astype(jnp.bfloat16),
        preferred_element_type=jnp.float32,
    )
    return product.astype(jnp.int32)


def ring_plan(schedules, seq, most_done, owner_ref, order_ref, plan_ref, found_ref):
    blocks = owner_ref.shape[0]
    capacity = order_ref.shape[1]
    shape = (blocks, seq)
    me = lax.axis_index("seq")
    down = lax.broadcasted_iota(jnp.int32, shape, 0)
    across = lax.broadcasted_iota(jnp.int32, shape, 1)
    from_lane = lax.broadcasted_iota(jnp.int32, (seq, seq), 0)
    to_lane = lax.broadcasted_iota(jnp.int32, (seq, seq), 1)
    owner = owner_ref[...]
    ahead = owner - across
    ahead = jnp.where(ahead < 0, ahead + seq, ahead)
    key = ahead * blocks + down
    order = jnp.zeros(shape, jnp.int32)
    for b in range(blocks):
        order = order + (key[b : b + 1] < key).astype(jnp.int32)
    moved = ahead > 0

    def routed(split):
        right = ahead <= split
        rightward = count_of(right, 0)
        slot = jnp.where(right, rightward - 1 - order, order - rightward)
        steps = jnp.where(moved, jnp.where(right, ahead, seq - ahead), 0)
        return slot, steps, right.astype(jnp.int32)

    best, cost = None, None
    for split in SPLITS:
        now = routed(split)
        share = (now[0] + 1).astype(jnp.float32) / (21 - now[1]).astype(jnp.float32)
        spent = jnp.max(jnp.where(moved, share, 0.0), axis=0, keepdims=True) + 0.002 * jnp.sum(
            now[1].astype(jnp.float32), axis=0, keepdims=True
        )
        spent = jnp.broadcast_to(spent, shape)
        if best is None:
            best, cost = now, spent
        else:
            less = spent < cost
            best = tuple(jnp.where(less, n, f) for n, f in zip(now, best))
            cost = jnp.where(less, spent, cost)

    mine = owner == me
    hot = mine.astype(jnp.float32)
    earlier = jnp.zeros(shape, jnp.float32)
    for b in range(blocks - 1):
        earlier = earlier + jnp.where(down > b, hot[b : b + 1], 0.0)
    each = jnp.broadcast_to(jnp.sum(hot, axis=0, keepdims=True), shape)
    rank = earlier.astype(jnp.int32) + whole_dot(each, from_lane < to_lane)
    row = jnp.full(shape, -1, jnp.int32)
    for k in range(capacity):
        row = jnp.where(mine & (rank == k), order_ref[me, k], row)

    def here(spot):
        return total_of(across == me, spot + 1, 1) - 1

    tier = jnp.zeros((1, 1), jnp.int32)
    for number, (first, second, slots) in enumerate(schedules):
        slot, steps, right = best if second else routed(seq // 2)
        wide, total = first[0], sum(first) + sum(second)
        wide_two = second[0] if second else 0
        turn = len(first)
        base = blocks + 1 + 2 * wide + 2 * wide_two
        at = base + jnp.where(right > 0, 0, total) + begun(first, steps) + slot
        sent = moved
        picks = jnp.zeros((1, seq), jnp.int32)
        fits = (most_done <= slots).astype(jnp.int32)
        if second:
            sent = moved & (slot < wide)
            for way in range(2):
                chosen = moved & (right == 1 - way)
                shift = to_lane - from_lane if way == 0 else from_lane - to_lane
                shifted = jnp.where(shift < 0, shift + seq, shift) == turn
                unshift = from_lane - to_lane if way == 0 else to_lane - from_lane
                unshifted = jnp.where(unshift < 0, unshift + seq, unshift) == turn
                on = chosen & sent & (steps > turn)
                left_on = whole_dot(jnp.where(on, steps - turn, 0), shifted)
                slot_on = whole_dot(jnp.where(on, slot, 0), shifted)
                left_late = jnp.where(chosen & (slot >= wide), steps, 0)
                key_on = left_on * (2 * blocks) + down
                key_late = left_late * (2 * blocks) + down + blocks
                rank_on = jnp.zeros(shape, jnp.int32)
                rank_late = jnp.zeros(shape, jnp.int32)
                for keys in (key_on, key_late):
                    for b in range(blocks):
                        rank_on = rank_on + (keys[b : b + 1] > key_on).astype(jnp.int32)
                        rank_late = rank_late + (keys[b : b + 1] > key_late).astype(jnp.int32)
                for left, place in ((left_on, rank_on), (left_late, rank_late)):
                    excess = jnp.where(left > 0, left - travel(second, place), 0)
                    excess = jnp.max(jnp.max(excess, axis=0, keepdims=True), axis=1, keepdims=True)
                    fits = fits * (excess <= 0).astype(jnp.int32)
                start = base + way * total + sum(first)
                rank_back = whole_dot(jnp.where(left_on > 0, rank_on, 0), unshifted)
                at = jnp.where(on, start + begun(second, steps - turn) + rank_back, at)
                at = jnp.where(left_late > 0, start + begun(second, left_late) + rank_late, at)
                for left, place, source in (
                    (left_on, rank_on, blocks + way * wide + slot_on),
                    (left_late, rank_late, down),
                ):
                    spot = here(jnp.where(left > 0, way * wide_two + place, -1))
                    value = here(source)
                    picks = picks + total_of(spot == across, jnp.broadcast_to(value, shape), 0)
        if number < len(schedules) - 1:
            tier = tier + 1 - fits
        at = jnp.where(moved, at, down)
        for c in range(capacity):
            found_ref[c : c + 1] = total_of(row == c, at + 1, 0)
        found = jnp.sum(found_ref[...], axis=1, keepdims=True)
        square = (capacity, capacity)
        diagonal = lax.broadcasted_iota(jnp.int32, square, 0) == lax.broadcasted_iota(jnp.int32, square, 1)
        source = total_of(diagonal, jnp.broadcast_to(found, square), 0)
        spot = here(jnp.where(sent, jnp.where(right > 0, 0, wide) + slot, -1))
        line = 3 * number
        plan_ref[line : line + 1, 0:seq] = total_of(spot == across, down, 0)
        plan_ref[line + 1 : line + 2, 0:capacity] = jnp.where(source > 0, source - 1, blocks)
        plan_ref[line + 2 : line + 3, 0:seq] = picks
    return tier


def exchange_kernel(
    tp, sub, groups, seq, requests, schedules,
    x_ref, owner_ref, length_ref, order_ref, query_ref, own_ref, tier_ref, plan_ref, table_ref, heads_ref,
    found, tiers, sem, send_sem, recv_sem, tier_send, tier_recv,
):
    group = lax.axis_index("groups")
    parts = head_parts(tp, sub, 0, x_ref, own_ref, sem, send_sem, recv_sem)
    others = [{"groups": lax.rem(group + step, groups)} for step in range(1, groups)]
    barrier = pltpu.get_barrier_semaphore()
    for where in head_peers(tp, sub) + others:
        pl.semaphore_signal(barrier, inc=1, device_id=where, device_id_type=MESH)
    pl.semaphore_wait(barrier, tp * sub + groups - 2)
    for part in parts:
        part.start()
    for head in range(heads_ref.shape[1]):
        heads_ref[:, head] = query_ref[:, head * HD : (head + 1) * HD].astype(jnp.float32)
    blocks = x_ref.shape[0]
    most_done = request_plan(blocks, seq, requests, length_ref, table_ref)
    tier = ring_plan(schedules, seq, most_done, owner_ref, order_ref, plan_ref, found)
    tiers[0] = jnp.broadcast_to(tier, tiers.shape[1:])
    told = [
        pltpu.make_async_remote_copy(
            src_ref=tiers.at[0],
            dst_ref=tiers.at[step + 1],
            send_sem=tier_send.at[step],
            recv_sem=tier_recv.at[step],
            device_id=where,
            device_id_type=MESH,
        )
        for step, where in enumerate(others)
    ]
    for part in told:
        part.start()
    for part in told + parts:
        part.wait()
    agreed = tiers[0]
    for step in range(len(others)):
        agreed = jnp.maximum(agreed, tiers[step + 1])
    tier_ref[0] = jnp.max(agreed)


def head_peers(tp, sub):
    me = lax.axis_index("tp") * sub + lax.axis_index("sub")
    others = [lax.rem(me + step, tp * sub) for step in range(1, tp * sub)]
    return [{"tp": other // sub, "sub": lax.rem(other, sub)} for other in others]


def head_parts(tp, sub, half, x_ref, own_ref, sem, send_sem, recv_sem):
    width = own_ref.shape[2]
    rows = x_ref.shape[2]
    me = lax.axis_index("tp") * sub + lax.axis_index("sub")
    mine = pl.ds(pl.multiple_of(me * rows, rows), rows)
    target = own_ref.at[:, mine, :]
    parts = [
        pltpu.make_async_copy(
            x_ref.at[:, half, :, pl.ds(pl.multiple_of(me * width, width), width)], target, sem
        )
    ]
    for step, where in enumerate(head_peers(tp, sub)):
        other = where["tp"] * sub + where["sub"]
        parts.append(
            pltpu.make_async_remote_copy(
                src_ref=x_ref.at[:, half, :, pl.ds(pl.multiple_of(other * width, width), width)],
                dst_ref=target,
                send_sem=send_sem.at[step],
                recv_sem=recv_sem.at[step],
                device_id=where,
                device_id_type=MESH,
            )
        )
    return parts


def exchange(prefill_kv, owners, lengths, slot_order, queries, schedules, tp, sub, groups, seq):
    blocks, _, rows, columns = prefill_kv.shape
    capacity = slot_order.shape[1]
    count = tp * sub
    requests = queries.shape[0]
    vmem = pl.BlockSpec(memory_space=pltpu.VMEM)
    return pl.pallas_call(
        functools.partial(exchange_kernel, tp, sub, groups, seq, requests, schedules),
        out_shape=(
            jax.ShapeDtypeStruct((blocks, rows * count, columns // count), prefill_kv.dtype),
            jax.ShapeDtypeStruct((1,), jnp.int32),
            jax.ShapeDtypeStruct((16, LANES), jnp.int32),
            jax.ShapeDtypeStruct((16, LANES), jnp.int32),
            jax.ShapeDtypeStruct((requests, queries.shape[1] // HD, HD), jnp.float32),
        ),
        in_specs=[pl.BlockSpec(memory_space=pl.ANY), vmem, vmem, pl.BlockSpec(memory_space=pltpu.SMEM), vmem],
        out_specs=[vmem, pl.BlockSpec(memory_space=pltpu.SMEM), vmem, vmem, vmem],
        scratch_shapes=[
            pltpu.VMEM((capacity, seq), jnp.int32),
            pltpu.VMEM((groups, 8, LANES), jnp.int32),
            pltpu.SemaphoreType.DMA,
            pltpu.SemaphoreType.DMA((count,)),
            pltpu.SemaphoreType.DMA((count,)),
            pltpu.SemaphoreType.DMA((groups,)),
            pltpu.SemaphoreType.DMA((groups,)),
        ],
        compiler_params=pltpu.CompilerParams(collective_id=0, has_side_effects=True),
    )(prefill_kv, owners, lengths, slot_order, queries)


def ring_kernel(
    first, second, slots, number, tp, sub, seq,
    x_ref, keys_ref, query_ref, new_ref, plan_ref, table_ref, cache_ref, rows_ref,
    klog, vlog, pool, values, gathered, alog, states, came, sem, head_send, head_recv, send_sem, recv_sem, asend_sem, arecv_sem,
    state_send, state_recv,
):
    me = lax.axis_index("seq")

    def along(step):
        return {"seq": lax.rem(me + step + seq, seq)}

    blocks = keys_ref.shape[0]
    capacity, requests = cache_ref.shape[0], rows_ref.shape[0]
    group_size = query_ref.shape[1]
    used, repack = first + second, len(first)
    total = sum(used)
    starts = [sum(used[:k]) for k in range(len(used))]
    line = 3 * number
    wide = {0: first[0]}
    stage = {0: blocks + 1}
    free = blocks + 1 + 2 * first[0]
    if second:
        wide[repack], stage[repack] = second[0], free
        free = free + 2 * second[0]
    base = (free, free + total)
    reach = (seq // 2, seq - 1 - seq // 2)
    logs = (klog, vlog)

    def stage_half(half, own_ref):
        log = logs[half]
        log[blocks] = jnp.zeros(log.shape[1:], log.dtype)

        def keep(i, carry):
            log[i] = own_ref[i]
            if second:
                pool[half, i] = own_ref[i]
            return carry

        lax.fori_loop(0, blocks, keep, 0)

        def pick(i, carry):
            log[stage[0] + i] = own_ref[plan_ref[line, i]]
            return carry

        lax.fori_loop(0, 2 * wide[0], pick, 0)

    def repack_half(half):
        log, step = logs[half], repack - 1

        def gather(i, carry):
            for way in range(2):
                block_copy(half, way, step, i).wait_recv()
                pool[half, blocks + way * used[step] + i] = log[base[way] + starts[step] + i]
            return carry

        lax.fori_loop(0, used[step], gather, 0)

        def pick(i, carry):
            log[stage[repack] + i] = pool[half, plan_ref[line + 2, i]]
            return carry

        lax.fori_loop(0, 2 * wide[repack], pick, 0)

    def block_copy(half, way, step, i):
        at = starts[step] + i
        if step in stage:
            source = stage[step] + way * wide[step] + i
        else:
            source = base[way] + starts[step - 1] + i
        return pltpu.make_async_remote_copy(
            src_ref=logs[half].at[source],
            dst_ref=logs[half].at[base[way] + at],
            send_sem=send_sem.at[half, way],
            recv_sem=recv_sem.at[half, way, at],
            device_id=along((1, -1)[way]),
            device_id_type=MESH,
        )

    def hop(half, step, low, high):
        def body(i, carry):
            for way in range(2):
                if step not in stage:
                    block_copy(half, way, step - 1, i).wait_recv()
                block_copy(half, way, step, i).start()
            return carry

        if low < high:
            lax.fori_loop(low, high, body, 0)

    express, doubled = 2, 4
    turns = len(used)
    if second:
        turns = repack + max(sum(n > express for n in second), len(second) - doubled)

    def forward(half, turn):
        if turn > 0 and turn in stage:
            repack_half(half)
        if not second or turn < repack:
            hop(half, turn, 0, used[turn])
            return
        late = turn - repack
        step = repack + late + min(late, doubled)
        if step < len(used):
            hop(half, step, 0, min(express, used[step]))
        if turn < len(used):
            hop(half, turn, express, used[turn])
        if late < doubled and step + 1 < len(used):
            hop(half, step + 1, 0, min(express, used[step + 1]))

    def land(half, step):
        beyond = used[step + 1] if step + 1 < len(used) else 0
        if step + 1 in stage:
            beyond = used[step]

        def body(i, carry):
            for way in range(2):
                block_copy(half, way, step, i).wait_recv()
            return carry

        lax.fori_loop(beyond, used[step], body, 0)

    def row_copy(way, step):
        at = way * reach[0] + step + 1
        source = 0 if step == 0 else at - 1
        return pltpu.make_async_remote_copy(
            src_ref=alog.at[pl.ds(source * slots, slots)],
            dst_ref=alog.at[pl.ds(at * slots, slots)],
            send_sem=asend_sem.at[at],
            recv_sem=arecv_sem.at[at],
            device_id=along((1, -1)[way]),
            device_id_type=MESH,
        )

    def state_copy(step):
        return pltpu.make_async_remote_copy(
            src_ref=states.at[blocks - 1],
            dst_ref=came.at[step],
            send_sem=state_send.at[step],
            recv_sem=state_recv.at[step],
            device_id=along(step + 1),
            device_id_type=MESH,
        )

    barrier = pltpu.get_barrier_semaphore()
    met = head_peers(tp, sub) + [along(step) for step in (1, -1, 2, -2)]
    for where in met:
        pl.semaphore_signal(barrier, inc=1, device_id=where, device_id_type=MESH)
    stage_half(0, keys_ref)
    pl.semaphore_wait(barrier, len(met))

    parts = head_parts(tp, sub, 1, x_ref, values, sem, head_send, head_recv)
    for part in parts:
        part.start()
    forward(0, 0)

    scale = HD ** (-0.5)
    token = lax.broadcasted_iota(jnp.int32, (group_size, BLOCK), 1)
    weights, peaks, sums = [], [], []
    for b in range(blocks):
        query = query_ref[table_ref[2, b]].astype(jnp.bfloat16)
        score = scale * lax.dot_general(
            query, keys_ref[b], (((1,), (1,)), ((), ())), preferred_element_type=jnp.float32
        )
        score = jnp.where(token < table_ref[3, b], score, NEG_FLOOR)
        peak = jnp.max(score, axis=1, keepdims=True)
        weight = jnp.exp(score - peak).astype(jnp.bfloat16)
        weights.append(weight)
        peaks.append(jnp.broadcast_to(peak, (group_size, HD)))
        sums.append(
            jnp.broadcast_to(
                jnp.sum(weight.astype(jnp.float32), axis=1, keepdims=True), (group_size, HD)
            )
        )

    def merge(first, second):
        top = jnp.maximum(first[0], second[0])
        one, two = jnp.exp(first[0] - top), jnp.exp(second[0] - top)
        return (top, one * first[1] + two * second[1], one * first[2] + two * second[2])

    def attend():
        state = None
        for b in range(blocks):
            partial = jnp.dot(weights[b], values[b], preferred_element_type=jnp.float32)
            fresh = (peaks[b], sums[b], partial)
            if state is not None:
                begins = table_ref[4, b] > 0
                joined = merge(state, fresh)
                fresh = tuple(jnp.where(begins, f, j) for f, j in zip(fresh, joined))
            state = fresh
            for part in range(3):
                states[b, part] = state[part]

    def answer(j, carry):
        request = table_ref[5, j]
        block = table_ref[6, j]
        state = tuple(states[block, part] for part in range(3))
        for back in range(2):
            enters = table_ref[7 + back, j] > 0
            joined = merge(state, tuple(came[back, part] for part in range(3)))
            state = tuple(jnp.where(enters, f, s) for f, s in zip(joined, state))
        new = new_ref[request].astype(jnp.float32)
        own = scale * jnp.sum(
            query_ref[request] * new[0:1], axis=1, keepdims=True
        )
        own = jnp.broadcast_to(own, (group_size, HD))
        ones = jnp.ones((group_size, HD), jnp.float32)
        _, denom, numer = merge(state, (own, ones, jnp.broadcast_to(new[1:2], (group_size, HD))))
        alog[j] = (numer / denom).astype(alog.dtype)
        return carry

    def row_hop(step):
        for way in range(2):
            if step < reach[way]:
                if step > 0:
                    row_copy(way, step - 1).wait_recv()
                row_copy(way, step).start()

    lag, rows_sent = 3, 0
    for turn in range(turns + 1):
        if 0 < turn < turns:
            forward(0, turn)
        if second and repack <= turn < turns and rows_sent < reach[0]:
            row_hop(rows_sent)
            rows_sent += 1
        if turn == 1:
            for part in parts:
                part.wait()
            stage_half(1, values)
        if 0 < turn <= turns:
            forward(1, turn - 1)
        if turn == 1:
            attend()
        if turn == 2:
            for step in range(2):
                state_copy(step).start()
        if turn == lag:
            for step in range(2):
                state_copy(step).wait()
            lax.fori_loop(0, slots, answer, 0)
        if turn >= lag and rows_sent < reach[0]:
            row_hop(rows_sent)
            rows_sent += 1
    for step in range(rows_sent, reach[0]):
        row_hop(step)

    for half in range(2):
        for step in range(len(used)):
            land(half, step)

        def place(c, carry, half=half):
            cache_ref[c, half] = logs[half][plan_ref[line + 1, c]]
            return carry

        lax.fori_loop(0, capacity, place, 0)
        if half == 0:
            for way in range(2):
                row_copy(way, reach[way] - 1).wait_recv()

            def collect(r, carry):
                gathered[r] = alog[table_ref[0, r] * slots + table_ref[1, r]].astype(jnp.float32)
                return carry

            lax.fori_loop(0, requests, collect, 0)
            for head in range(group_size):
                rows_ref[:, head * HD : (head + 1) * HD] = gathered[:, head].astype(rows_ref.dtype)
    for way in range(2):
        for step in range(reach[way]):
            row_copy(way, step).wait_send()
        for half in range(2):
            every = logs[half].at[pl.ds(base[way], total)]
            pltpu.make_async_remote_copy(
                src_ref=every,
                dst_ref=every,
                send_sem=send_sem.at[half, way],
                recv_sem=recv_sem.at[half, way, 0],
                device_id=along((1, -1)[way]),
                device_id_type=MESH,
            ).wait_send()

def ring(first, second, slots, number, tp, sub, seq, capacity, prefill_kv, keys, queries, new_kv, plan, table):
    blocks = keys.shape[0]
    staged, total = first[0] + sum(second[:1]), sum(first) + sum(second)
    requests, group_size = queries.shape[:2]
    count = tp * sub
    vmem = pl.BlockSpec(memory_space=pltpu.VMEM)
    smem = pl.BlockSpec(memory_space=pltpu.SMEM)
    log = pltpu.VMEM((blocks + 1 + 2 * staged + 2 * total,) + keys.shape[1:], keys.dtype)
    return pl.pallas_call(
        functools.partial(ring_kernel, first, second, slots, number, tp, sub, seq),
        out_shape=(
            jax.ShapeDtypeStruct((capacity, 2) + keys.shape[1:], keys.dtype),
            jax.ShapeDtypeStruct((requests, group_size * HD), jnp.bfloat16),
        ),
        in_specs=[pl.BlockSpec(memory_space=pl.ANY), vmem, vmem, vmem, smem, smem],
        out_specs=(vmem, vmem),
        scratch_shapes=[
            log,
            log,
            pltpu.VMEM((2, blocks + 2 * first[-1]) + keys.shape[1:], keys.dtype),
            pltpu.VMEM(keys.shape, keys.dtype),
            pltpu.VMEM((requests, group_size, HD), jnp.float32),
            pltpu.VMEM((seq * slots, group_size, HD), jnp.bfloat16),
            pltpu.VMEM((blocks, 3, group_size, HD), jnp.float32),
            pltpu.VMEM((2, 3, group_size, HD), jnp.float32),
            pltpu.SemaphoreType.DMA,
            pltpu.SemaphoreType.DMA((count,)),
            pltpu.SemaphoreType.DMA((count,)),
            pltpu.SemaphoreType.DMA((2, 2)),
            pltpu.SemaphoreType.DMA((2, 2, total)),
            pltpu.SemaphoreType.DMA((seq,)),
            pltpu.SemaphoreType.DMA((seq,)),
            pltpu.SemaphoreType.DMA((2,)),
            pltpu.SemaphoreType.DMA((2,)),
        ],
        compiler_params=pltpu.CompilerParams(
            collective_id=number + 1, has_side_effects=True, vmem_limit_bytes=60 << 20
        ),
    )(prefill_kv, keys, queries, new_kv, plan, table)


def travel(used, slot):
    return sum((slot < n).astype(jnp.int32) for n in used)


def per_device(tp, sub, groups, seq, prefill_kv, prompt_lengths, block_owner, slot_order, queries, new_kv):
    shard_blocks = prefill_kv.shape[0]
    capacity = slot_order.shape[1]
    schedules = tiers(shard_blocks, seq)
    owners = block_owner.reshape(seq, shard_blocks).T
    keys, agreed, plan, table, query_rows = exchange(
        prefill_kv, owners, prompt_lengths[None], slot_order, queries, schedules, tp, sub, groups, seq
    )

    def deliver(number):
        first, second, slots = schedules[number]
        return ring(
            first, second, slots, number, tp, sub, seq, capacity,
            prefill_kv, keys, query_rows, new_kv, plan, table,
        )

    decode_cache, rows = lax.switch(
        agreed.reshape(()), [functools.partial(deliver, number) for number in range(len(schedules))]
    )
    return (decode_cache, rows)


def solution(mesh):
    return jax.shard_map(
        functools.partial(
            per_device, mesh.shape["tp"], mesh.shape["sub"], mesh.shape["groups"], mesh.shape["seq"]
        ),
        mesh=mesh,
        in_specs=(
            P(("groups", "seq"), None, ("tp", "sub"), None),
            P("groups"),
            P("groups"),
            P("groups", None),
            P("groups", ("tp", "sub")),
            P("groups", None, ("tp", "sub")),
        ),
        out_specs=(P(("groups", "seq"), None, None, ("tp", "sub")), P("groups", ("tp", "sub"))),
        check_vma=False,
    )
```
